256 devices in a mesh: parts: 256 (over y, x, z, core).
Axes of the slice: x: 4, y: 4, z: 8, core: 2. Of those that a mesh axis runs over, the one named last changes fastest.
Arguments:
- basis: float32 [16, 262144], P(None, 'parts'), may hold values from -8000 to 8000, as said below
- k_tiles: float32 [2048, 5, 128, 128], P('parts'), may hold values from -3 to 11, as said below
- m_tiles: float32 [2048, 5, 128, 128], P('parts'), may hold values from -2 to 4, as said below
- tile_part: int32 [2048, 5], P('parts'), may hold values from 0 to 255, as said below
- tile_slot: int32 [2048, 5], P('parts'), may hold values from 0 to 7, as said below
- iface_rows: int32 [512], P('parts'), may hold values from 0 to 7
Outputs:
- corrections: float32 [16, 262144], P(None, 'parts')
- theta: float32 [16], replicated
The draws below stay inside these ranges and needn't reach their ends.
Inputs may be any that keep to these rules, and one draw needn't show every extreme that they name: `basis`: the rows form a full-rank set. `k_tiles`: block 0 of every row tile has a positive diagonal well above its other entries. `m_tiles`: block 0 of every row tile has a positive diagonal. `tile_part`: block 0 of a row tile lies in its own partition; every other block lies in its own partition, in the partition 1 away on either side, or in the partition 128 away, counted modulo the number of partitions. `tile_slot`: where the block lies in the own partition this is a row tile of it (for block 0 the row tile itself); elsewhere an interface slot below 2.
All inputs are finite; a program needn't handle non-finite values.
Results may differ from the reference program's by a relative error of at most 0.0003.
Values sent between devices are 32-bit elements; how exact they have to be, the bound alone decides.
A program may use at most 64 MiB of HBM per device.

```python
import jax
import jax.numpy as jnp
from jax import lax

PAIRS = 16
TILE = 128
BLOCKS = 5
STEPS = 4
IFACE = 2
TILES_DEV = 8
STRIDE = 128
ROW_TILES = 2048
ROWS = 262144
N_PARTS = 256


def draw_basis(key, part):
    keys = jax.random.split(key, 3)
    values = jax.random.truncated_normal(keys[0], -5.0, 5.0, (PAIRS, ROWS), jnp.float32)
    power = 1.0
    column_scale = jnp.exp(jax.random.uniform(keys[1], (PAIRS, 1), jnp.float32, 0.0, 2.3026))
    tile_scale = jnp.exp(jax.random.uniform(keys[2], (1, ROW_TILES), jnp.float32, 0.0, 2.3026))
    tile_scale = jnp.repeat(tile_scale, TILE, axis=1)
    place = (jnp.arange(ROWS, dtype=jnp.int32) // (TILES_DEV * TILE)).astype(jnp.float32)
    ramp = (3.0 ** (place / (N_PARTS - 1))) ** power
    return values * column_scale * tile_scale * ramp[None, :]


def operator_like(key, ratio, lowest, highest):
    keys = jax.random.split(key, 2)
    spread = ratio / (BLOCKS * TILE) ** 0.5
    shape = (ROW_TILES, BLOCKS, TILE, TILE)
    entries = jax.random.truncated_normal(keys[0], -5.0, 5.0, shape, jnp.float32) * spread
    diagonal = jax.random.uniform(keys[1], (ROW_TILES, TILE), jnp.float32, lowest, highest)
    eye = jnp.eye(TILE, dtype=jnp.float32)
    return entries.at[:, 0].add(diagonal[:, :, None] * eye[None])


def draw_k_tiles(key, part):
    return operator_like(jax.random.fold_in(key, 11), 3.0, 4.0, 8.0)


def draw_m_tiles(key, part):
    return operator_like(jax.random.fold_in(key, 13), 0.75, 1.0, 2.0)


def tile_pattern(key):
    keys = jax.random.split(jax.random.fold_in(key, 7), 4)
    shape = (ROW_TILES, BLOCKS)
    owner = (jnp.arange(ROW_TILES, dtype=jnp.int32) // TILES_DEV)[:, None]
    own_tile = (jnp.arange(ROW_TILES, dtype=jnp.int32) % TILES_DEV)[:, None]
    first = jnp.arange(BLOCKS, dtype=jnp.int32)[None, :] == 0
    coin = jax.random.randint(keys[0], shape, 0, 2) == 1
    remote = jnp.logical_and(coin, jnp.logical_not(first))
    direction = jax.random.randint(keys[1], shape, 0, 4)
    offsets = jnp.where(direction == 0, 1, jnp.where(direction == 1, -1, jnp.where(direction == 2, STRIDE, -STRIDE)))
    neighbour = (owner + offsets + N_PARTS) % N_PARTS
    local_slot = jax.random.randint(keys[2], shape, 0, TILES_DEV)
    iface_slot = jax.random.randint(keys[3], shape, 0, IFACE)
    parts_of = jnp.where(remote, neighbour, owner + 0 * neighbour)
    slots = jnp.where(remote, iface_slot, jnp.where(first, own_tile + 0 * local_slot, local_slot))
    return (parts_of.astype(jnp.int32), slots.astype(jnp.int32))


def draw_tile_part(key, part):
    return tile_pattern(key)[0]


def draw_tile_slot(key, part):
    return tile_pattern(key)[1]


def with_ends(result, stream_key, least, largest):
    longest = result.shape.index(max(result.shape))
    spots = []
    for shift in (0, 1):
        where = [jax.random.randint(jax.random.fold_in(stream_key, axis), (), 0, length) for axis, length in enumerate(result.shape)]
        where[longest] = (where[longest] + shift) % result.shape[longest]
        spots.append(tuple(where))
    return result.at[spots[0]].set(least).at[spots[1]].set(largest)


def setup_inputs(seed: int = 0) -> dict:
    key_list = jax.random.split(jax.random.key(seed), 7)
    basis = draw_basis(jax.random.fold_in(key_list[6], 71), 0)
    k_tiles = draw_k_tiles(jax.random.fold_in(key_list[6], 71), 0)
    m_tiles = draw_m_tiles(jax.random.fold_in(key_list[6], 71), 0)
    tile_part = draw_tile_part(jax.random.fold_in(key_list[6], 71), 0)
    tile_slot = draw_tile_slot(jax.random.fold_in(key_list[6], 71), 0)
    iface_rows = with_ends(jax.random.randint(key_list[5], (N_PARTS * IFACE,), 0, TILES_DEV), jax.random.fold_in(key_list[5], 1), 0, TILES_DEV - 1).astype(jnp.int32)
    return {"basis": basis, "k_tiles": k_tiles, "m_tiles": m_tiles, "tile_part": tile_part, "tile_slot": tile_slot, "iface_rows": iface_rows}


relax = 0.4

def product(left, right):
    return jnp.dot(left.astype(jnp.float32), right.astype(jnp.float32), precision=lax.Precision.HIGHEST, preferred_element_type=jnp.float32)

def inverse_lower(chol):
    eye = jnp.eye(chol.shape[0], dtype=chol.dtype)
    return jax.scipy.linalg.solve_triangular(chol, eye, lower=True)

def apply_pair(vectors, k_tiles, m_tiles, columns):
    blocks = vectors.reshape(PAIRS, ROW_TILES, TILE)
    picked = jnp.take(blocks, columns, axis=1)
    stiff = jnp.einsum('ptbc,tbrc->ptr', picked, k_tiles, precision=lax.Precision.HIGHEST)
    mass = jnp.einsum('ptbc,tbrc->ptr', picked, m_tiles, precision=lax.Precision.HIGHEST)
    return (stiff.reshape(PAIRS, ROWS), mass.reshape(PAIRS, ROWS))

def reference(basis, k_tiles, m_tiles, tile_part, tile_slot, iface_rows):
    owner = (jnp.arange(ROW_TILES, dtype=jnp.int32) // TILES_DEV)[:, None]
    lookup = jnp.clip(tile_part * IFACE + tile_slot, 0, N_PARTS * IFACE - 1).astype(jnp.int32)
    remote_tile = jnp.take(iface_rows, lookup)
    columns = (tile_part * TILES_DEV + jnp.where(tile_part == owner, tile_slot, remote_tile)).astype(jnp.int32)
    gram = product(basis, basis.T) / ROWS
    inv_v = inverse_lower(jnp.linalg.cholesky(gram))
    ortho = product(inv_v, basis)
    k_ortho, m_ortho = apply_pair(ortho, k_tiles, m_tiles, columns)
    mass_gram = product(m_ortho, m_ortho.T) / ROWS
    stiff_cross = product(m_ortho, k_ortho.T) / ROWS
    chol_b = jnp.linalg.cholesky(mass_gram)
    inv_b = inverse_lower(chol_b)
    test_basis = product(inv_b, m_ortho)
    theta = jnp.diagonal(product(inv_b, stiff_cross)) / jnp.diagonal(chol_b)
    resid = k_ortho - theta[:, None] * m_ortho
    diag_k = jnp.diagonal(k_tiles[:, 0], axis1=1, axis2=2).reshape(ROWS)
    correct = -relax * resid / diag_k
    for step in range(STEPS):
        right = product(correct, ortho.T) / ROWS
        moved = correct - product(right, ortho)
        k_moved, m_moved = apply_pair(moved, k_tiles, m_tiles, columns)
        image = k_moved - theta[:, None] * m_moved
        left = product(image, test_basis.T) / ROWS
        image = image - product(left, test_basis)
        correct = correct - relax * (resid + image) / diag_k
    final = product(correct, ortho.T) / ROWS
    correct = correct - product(final, ortho)
    return (correct, theta)
```

```python
import functools

import jax
import jax.numpy as jnp
from jax import lax
from jax.experimental import pallas as pl
from jax.experimental.pallas import tpu as pltpu
from jax.sharding import PartitionSpec as P

AXIS = "parts"
PARTS = 256
GROUP = 16
FAR = 128
PAIRS = 16
TILES = 8
BLOCKS = 5
WIDTH = 128
LOCAL = TILES * WIDTH
EXT = TILES + 6
RELAX = 0.4
MESH = pl.DeviceIdType.MESH
F32 = jnp.float32
BF16 = jnp.bfloat16
NT = (((1,), (1,)), ((), ()))
TN = (((0,), (0,)), ((), ()))


def split(x):
    hi = x.astype(BF16)
    return hi, (x - hi.astype(F32)).astype(BF16)


def mm(a, b):
    return jnp.dot(a, b, preferred_element_type=F32)


def mm_nt(a, b):
    return lax.dot_general(a, b, NT, preferred_element_type=F32)


def small(a, b, dims=(((1,), (0,)), ((), ()))):
    return lax.dot_general(
        a, b, dims, precision=lax.Precision.HIGHEST, preferred_element_type=F32
    )


def pack4(v):
    return jnp.concatenate([v[4 * i : 4 * i + 4] for i in range(4)], axis=1)


def unpack4(v):
    return jnp.concatenate([v[:, 32 * i : 32 * i + 32] for i in range(4)], axis=0)


def eliminate(gram, rows, eye):
    aug = jnp.concatenate([gram, eye], axis=1)
    for j in range(PAIRS):
        pivot = aug[j : j + 1, j : j + 1]
        d = lax.rsqrt(pivot)
        d = d * (1.5 - 0.5 * pivot * d * d)
        line = aug[j : j + 1, :] * d
        col = aug[:, j : j + 1] * d
        aug = jnp.where(rows == j, line, jnp.where(rows > j, aug - col * line, aug))
    return aug[:, PAIRS:]


def kernel(
    scale,
    basis_ref,
    k_ref,
    m_ref,
    part_ref,
    slot_ref,
    iface_ref,
    out_ref,
    theta_ref,
    kbuf,
    mbuf,
    w_hi,
    w_lo,
    xt,
    dinv,
    ext16,
    ext32,
    words,
    words_r,
    s_hi,
    s_lo,
    pt,
    ad,
    right,
    left,
    h0out,
    h1out,
    h2out,
    h3out,
    h0in,
    h1in,
    h2in,
    h3in,
    ar_big,
    ar_small,
    load_sem,
    x_sem,
    hs_sem,
    hr_sem,
    as_sem,
    ar_sem,
):
    me = lax.axis_index(AXIS)
    rank_a = lax.rem(me, GROUP)
    base_a = me - rank_a
    rank_b = me // GROUP
    halo_to = (
        lax.rem(me + PARTS - 1, PARTS),
        lax.rem(me + 1, PARTS),
        lax.rem(me + FAR, PARTS),
    )

    def peer_a(k):
        return base_a + lax.rem(rank_a + k, GROUP)

    def peer_b(k):
        return rank_a + GROUP * lax.rem(rank_b + k, GROUP)

    loads = []
    for i in range(TILES):
        loads.append(
            pltpu.make_async_copy(
                basis_ref.at[:, pl.ds(i * WIDTH, WIDTH)], xt.at[i], x_sem.at[i]
            )
        )
        loads[-1].start()
    for i in range(TILES):
        for n, (src, dst) in enumerate(((k_ref, kbuf), (m_ref, mbuf))):
            pltpu.make_async_copy(src.at[i], dst.at[i], load_sem.at[n, i]).start()

    barrier = pltpu.get_barrier_semaphore()

    def greet(k, carry):
        pl.semaphore_signal(barrier, inc=1, device_id=(peer_a(k),), device_id_type=MESH)
        pl.semaphore_signal(barrier, inc=1, device_id=(peer_b(k),), device_id_type=MESH)
        return carry

    lax.fori_loop(1, GROUP, greet, 0)
    for device in halo_to:
        pl.semaphore_signal(barrier, inc=1, device_id=(device,), device_id_type=MESH)

    def halo(step, out, into):
        for g, device in enumerate(halo_to):
            pltpu.make_async_remote_copy(
                src_ref=out,
                dst_ref=into.at[g],
                send_sem=hs_sem.at[step],
                recv_sem=hr_sem.at[step],
                device_id=(device,),
                device_id_type=MESH,
            ).start()

    def halo_wait(step, into):
        pltpu.make_async_copy(into, into, hr_sem.at[step]).wait()

    def spread(buf, stage, step, value):
        rank = rank_a if stage == 0 else rank_b
        peer = peer_a if stage == 0 else peer_b
        buf[rank] = value

        def send(k, carry):
            pltpu.make_async_remote_copy(
                src_ref=buf.at[rank],
                dst_ref=buf.at[rank],
                send_sem=as_sem.at[2 * step + stage],
                recv_sem=ar_sem.at[2 * step + stage],
                device_id=(peer(k),),
                device_id_type=MESH,
            ).start()
            return carry

        lax.fori_loop(1, GROUP, send, 0)

    def gathered(buf, stage, step):
        most = buf.at[pl.ds(0, GROUP - 1)]
        pltpu.make_async_copy(most, most, ar_sem.at[2 * step + stage]).wait()
        total = buf[0]
        for j in range(1, GROUP):
            total = total + buf[j]
        return total

    columns = []
    for i in range(TILES):
        line = []
        for b in range(BLOCKS):
            part = part_ref[i, b]
            slot = slot_ref[i, b]
            where = jnp.where(
                part == halo_to[1],
                TILES,
                jnp.where(part == halo_to[0], TILES + 2, TILES + 4),
            )
            line.append(jnp.where(part == me, slot, where + slot))
        columns.append(line)
    iface = [iface_ref[0], iface_ref[1]]

    def span(i):
        return pl.ds(i * WIDTH, WIDTH)

    for copy in loads:
        copy.wait()
    for s in range(2):
        h0out[s] = xt[iface[s]]
    pl.semaphore_wait(barrier, 33)
    halo(0, h0out, h0in)

    eye_w = lax.broadcasted_iota(jnp.int32, (WIDTH, WIDTH), 0) == lax.broadcasted_iota(
        jnp.int32, (WIDTH, WIDTH), 1
    )
    for i in range(TILES):
        hi, lo = split(xt[i])
        ext16[i, 0:16] = hi
        ext16[i, 16:32] = lo
        right[64:80, span(i)] = hi
        right[80:96, span(i)] = lo
        left[0:16, span(i)] = hi
        left[48:64, span(i)] = lo

    def prepare(i, carry):
        for n, (src, dst) in enumerate(((k_ref, kbuf), (m_ref, mbuf))):
            pltpu.make_async_copy(src.at[i], dst.at[i], load_sem.at[n, i]).wait()
            for b in range(BLOCKS):
                hi, lo = split(dst[i, b].T)
                w_hi[i, b * WIDTH : (b + 1) * WIDTH, n * WIDTH : (n + 1) * WIDTH] = hi
                w_lo[i, b * WIDTH : (b + 1) * WIDTH, n * WIDTH : (n + 1) * WIDTH] = lo
        diagonal = jnp.sum(jnp.where(eye_w, kbuf[i, 0], 0.0), axis=0, keepdims=True)
        dinv[i] = jnp.broadcast_to(1.0 / diagonal, (8, WIDTH))
        return carry

    lax.fori_loop(0, TILES, prepare, 0)
    d = [dinv[i, 0:1] for i in range(TILES)]
    for i in range(TILES):
        hi, lo = split(xt[i] * d[i])
        right[16:32, span(i)] = hi
        right[48:64, span(i)] = lo

    def apply(ext, rows, i):
        picked = jnp.concatenate([ext[columns[i][b]] for b in range(BLOCKS)], axis=1)
        high = mm(picked, w_hi[i])
        low = mm(picked[:rows], w_lo[i])
        return high[:rows] + high[rows:] + low

    halo_wait(0, h0in)
    for g in range(3):
        for s in range(2):
            hi, lo = split(h0in[g, s])
            ext16[TILES + 2 * g + s, 0:16] = hi
            ext16[TILES + 2 * g + s, 16:32] = lo
    for i in range(TILES):
        y = apply(ext16, 16, i)
        p, q = y[:, :WIDTH], y[:, WIDTH:]
        words[i, 0:16] = p * d[i]
        words[i, 16:32] = q * d[i]
        hi, lo = split(p)
        left[16:32, span(i)] = hi
        left[64:80, span(i)] = lo
        hi, lo = split(q)
        left[32:48, span(i)] = hi
        left[80:96, span(i)] = lo
        right[0:16, span(i)] = hi
        right[32:48, span(i)] = lo
    for s in range(2):
        h1out[s] = words[iface[s], 0:32]
    halo(1, h1out, h1in)

    gram = mm_nt(left[0:96], right[...])
    gram = gram[0:48] + gram[48:96]
    with_qx = gram[:, 0:32] + gram[:, 32:64]
    with_x = gram[:, 64:80] + gram[:, 80:96]
    payload = jnp.concatenate(
        [with_qx[16:32], with_qx[32:48], with_x[0:16], jnp.zeros((16, 48), F32)], axis=1
    )
    spread(ar_big.at[0], 0, 0, payload)

    for i in range(TILES):
        hi, lo = split(words[i, 0:32])
        ext32[i, 0:32] = hi
        ext32[i, 32:64] = lo
        s_hi[i, 0:32] = hi
        s_lo[i, 0:32] = lo
    spread(ar_big.at[1], 1, 0, gathered(ar_big.at[0], 0, 0))
    halo_wait(1, h1in)
    for g in range(3):
        for s in range(2):
            hi, lo = split(h1in[g, s])
            t = TILES + 2 * g + s
            ext32[t, 0:32] = hi
            ext32[t, 32:64] = lo
            s_hi[t, 0:32] = hi
            s_lo[t, 0:32] = lo

    for i in range(TILES):
        y = apply(ext32, 32, i)
        stiff, mass = y[:, :WIDTH], y[:, WIDTH:]
        hi, lo = split(stiff)
        left[0:32, span(i)] = hi
        left[64:96, span(i)] = lo
        hi, lo = split(mass)
        left[32:64, span(i)] = hi
        left[96:128, span(i)] = lo
        stiff, mass = stiff * d[i], mass * d[i]
        words[i, 32:48] = stiff[16:32]
        words[i, 48:64] = mass[16:32]
        words[i, 64:80] = stiff[0:16]
        words[i, 80:96] = mass[0:16]
    for s in range(2):
        h2out[s] = words[iface[s], 32:96]
    halo(2, h2out, h2in)
    gram = mm_nt(left[...], right[0:64])
    gram = gram[0:64] + gram[64:128]
    gram = gram[:, 0:32] + gram[:, 32:64]
    payload = jnp.concatenate([gram[16 * r : 16 * r + 16] for r in range(4)], axis=1)
    spread(ar_big.at[2], 0, 1, payload)
    for i in range(TILES):
        hi, lo = split(words[i, 32:96])
        s_hi[i, 32:96] = hi
        s_lo[i, 32:96] = lo

    total = gathered(ar_big.at[1], 1, 0) * scale
    g_p, g_q, g_xx = total[:, 0:32], total[:, 32:64], total[:, 64:80]
    g_pq, g_px = g_p[:, 0:16], g_p[:, 16:32]
    g_qq, g_qx = g_q[:, 0:16], g_q[:, 16:32]
    row_no = lax.broadcasted_iota(jnp.int32, (PAIRS, 2 * PAIRS), 0)
    eye_b = lax.broadcasted_iota(jnp.int32, (PAIRS, PAIRS), 0) == lax.broadcasted_iota(
        jnp.int32, (PAIRS, PAIRS), 1
    )
    eye = jnp.where(eye_b, 1.0, 0.0).astype(F32)
    inv_v = eliminate(g_xx, row_no, eye)
    inv_m = eliminate(g_qq, row_no, eye)
    projected = small(inv_m, g_pq, NT)
    diag_v = jnp.sum(jnp.where(eye_b, inv_v, 0.0), axis=1, keepdims=True)
    diag_m = jnp.sum(jnp.where(eye_b, inv_m, 0.0), axis=1, keepdims=True)
    theta = jnp.sum(projected * inv_v, axis=1, keepdims=True) * diag_m / diag_v
    theta_ref[...] = jnp.sum(jnp.where(eye_b, theta, 0.0), axis=0, keepdims=True)
    wide = jnp.broadcast_to(theta, (PAIRS, WIDTH))
    gram_v = small(inv_v, inv_v, TN)
    gram_m = small(inv_m, inv_m, TN)
    start_p = -RELAX * inv_v
    start_q = RELAX * theta * inv_v
    start_x = small(start_p, g_px) + small(start_q, g_qx)
    r = small(start_x, gram_v)
    r_pq = small(r, g_pq)
    coef = jnp.concatenate(
        [
            2.0 * start_p + RELAX * r,
            2.0 * start_q,
            -RELAX * start_q,
            RELAX * theta * start_q,
            -RELAX * start_p,
            RELAX * theta * start_p,
        ],
        axis=1,
    )
    spread(ar_big.at[3], 1, 1, gathered(ar_big.at[2], 0, 1))
    halo_wait(2, h2in)
    for g in range(3):
        for s in range(2):
            hi, lo = split(h2in[g, s])
            t = TILES + 2 * g + s
            s_hi[t, 32:96] = hi
            s_lo[t, 32:96] = lo

    def combine(coef, rows, t):
        hi, lo = split(coef)
        both = jnp.concatenate([hi, lo], axis=0)
        first = mm(both, s_hi[t, 0:rows])
        second = mm(hi, s_lo[t, 0:rows])
        return first[0:16] + first[16:32] + second

    for t in range(EXT):
        p = combine(coef, 96, t)
        pt[t] = p
        hi, lo = split(p)
        ext16[t, 0:16] = hi
        ext16[t, 16:32] = lo

    def residual(step, last):
        for i in range(TILES):
            y = apply(ext16, 16, i)
            image = y[:, :WIDTH] - wide * y[:, WIDTH:]
            hi, lo = split(image)
            left[0:16, span(i)] = hi
            left[16:32, span(i)] = lo
            ad[i] = image * d[i]
        if not last:
            out = h3out.at[step - 1]
            for s in range(2):
                out[s] = ad[iface[s]]
            halo(step + 2, out, h3in.at[step - 1])
        gram = mm_nt(left[0:32], right[0:64])
        gram = gram[0:16] + gram[16:32]
        gram = gram[:, 0:32] + gram[:, 32:64]
        spread(ar_small.at[2 * step - 2], 0, step + 1, pack4(gram))

    residual(1, False)

    total = gathered(ar_big.at[3], 1, 1) * scale
    kq, mq = total[:, 32:64], total[:, 96:128]
    kp, mp = total[:, 0:32], total[:, 64:96]
    image = (small(start_p, kp) + small(start_q, kq)) - theta * (
        small(start_p, mp) + small(start_q, mq)
    )
    p_x = 2.0 * start_x - RELAX * image[:, 16:32] + RELAX * small(r, g_px)

    for step in (1, 2, 3):
        m = small(image[:, 0:16] - r_pq, gram_m)
        c_x = p_x + RELAX * small(m, g_qx)
        r = small(c_x, gram_v)
        m_image = RELAX * (small(m, kq) - theta * small(m, mq))
        coef = jnp.concatenate(
            [
                start_p + RELAX * r,
                start_q + RELAX * m,
                -RELAX * RELAX * m,
                RELAX * RELAX * theta * m,
            ],
            axis=1,
        )
        if step < 3:
            for t in range(TILES):
                p = pt[t] - RELAX * ad[t] + combine(coef, 64, t)
                pt[t] = p
                hi, lo = split(p)
                ext16[t, 0:16] = hi
                ext16[t, 16:32] = lo
            for t in range(TILES, EXT):
                pt[t] = pt[t] + combine(coef, 64, t)
            got = gathered(ar_small.at[2 * step - 2], 0, step + 1)
            spread(ar_small.at[2 * step - 1], 1, step + 1, got)
            halo_wait(step + 2, h3in.at[step - 1])
            for g in range(3):
                for s in range(2):
                    t = TILES + 2 * g + s
                    p = pt[t] - RELAX * h3in[step - 1, g, s]
                    pt[t] = p
                    hi, lo = split(p)
                    ext16[t, 0:16] = hi
                    ext16[t, 16:32] = lo
            residual(step + 1, step == 2)
        else:
            got = gathered(ar_small.at[2 * step - 2], 0, step + 1)
            spread(ar_small.at[2 * step - 1], 1, step + 1, got)
            for t in range(TILES):
                pt[t] = pt[t] - RELAX * ad[t] + combine(coef, 64, t)
        r_px = small(r, g_px)
        r_pq = small(r, g_pq)
        total = unpack4(gathered(ar_small.at[2 * step - 1], 1, step + 1)) * scale
        image = total + m_image
        p_x = c_x + start_x - RELAX * image[:, 16:32] + RELAX * r_px

    m = small(image[:, 0:16] - r_pq, gram_m)
    c_x = p_x + RELAX * small(m, g_qx)
    r = small(c_x, gram_v)
    q_hi, q_lo = split(RELAX * m)
    x_hi, x_lo = split(-r)
    lead = jnp.concatenate([q_hi, x_hi], axis=1)
    rest = jnp.concatenate([q_lo, x_lo], axis=1)
    for t in range(TILES):
        hi = jnp.concatenate([s_hi[t, 16:32], right[64:80, span(t)]], axis=0)
        lo = jnp.concatenate([s_lo[t, 16:32], right[80:96, span(t)]], axis=0)
        out_ref[:, span(t)] = pt[t] + (mm(lead, hi) + mm(rest, hi) + mm(lead, lo))

    for step, out in enumerate((h0out, h1out, h2out, h3out.at[0], h3out.at[1])):
        for g in range(3):
            pltpu.make_async_copy(out, out, hs_sem.at[step]).wait()
    for step in range(5):
        for stage in range(2):
            buf = ar_big.at[2 * step + stage] if step < 2 else ar_small.at[2 * step - 4 + stage]
            most = buf.at[pl.ds(0, GROUP - 1)]
            pltpu.make_async_copy(most, most, as_sem.at[2 * step + stage]).wait()


def shards(basis, k_tiles, m_tiles, tile_part, tile_slot, iface_rows):
    rows = basis.shape[1] * lax.axis_size(AXIS)
    vmem = pltpu.VMEM
    corrections, theta = pl.pallas_call(
        functools.partial(kernel, 1.0 / rows),
        out_shape=(
            jax.ShapeDtypeStruct((PAIRS, LOCAL), F32),
            jax.ShapeDtypeStruct((1, PAIRS), F32),
        ),
        in_specs=[pl.BlockSpec(memory_space=pl.ANY)] * 3
        + [pl.BlockSpec(memory_space=pltpu.SMEM)] * 3,
        out_specs=(pl.BlockSpec(memory_space=vmem), pl.BlockSpec(memory_space=vmem)),
        scratch_shapes=[
            vmem((TILES, BLOCKS, WIDTH, WIDTH), F32),
            vmem((TILES, BLOCKS, WIDTH, WIDTH), F32),
            vmem((TILES, BLOCKS * WIDTH, 2 * WIDTH), BF16),
            vmem((TILES, BLOCKS * WIDTH, 2 * WIDTH), BF16),
            vmem((TILES, 16, WIDTH), F32),
            vmem((TILES, 8, WIDTH), F32),
            vmem((EXT, 32, WIDTH), BF16),
            vmem((EXT, 64, WIDTH), BF16),
            vmem((TILES, 96, WIDTH), F32),
            vmem((8, WIDTH), F32),
            vmem((EXT, 96, WIDTH), BF16),
            vmem((EXT, 96, WIDTH), BF16),
            vmem((EXT, 16, WIDTH), F32),
            vmem((TILES, 16, WIDTH), F32),
            vmem((96, LOCAL), BF16),
            vmem((128, LOCAL), BF16),
            vmem((2, 16, WIDTH), F32),
            vmem((2, 32, WIDTH), F32),
            vmem((2, 64, WIDTH), F32),
            vmem((2, 2, 16, WIDTH), F32),
            vmem((3, 2, 16, WIDTH), F32),
            vmem((3, 2, 32, WIDTH), F32),
            vmem((3, 2, 64, WIDTH), F32),
            vmem((2, 3, 2, 16, WIDTH), F32),
            vmem((4, GROUP, 16, WIDTH), F32),
            vmem((6, GROUP, 4, WIDTH), F32),
            pltpu.SemaphoreType.DMA((2, TILES)),
            pltpu.SemaphoreType.DMA((TILES,)),
            pltpu.SemaphoreType.DMA((5,)),
            pltpu.SemaphoreType.DMA((5,)),
            pltpu.SemaphoreType.DMA((10,)),
            pltpu.SemaphoreType.DMA((10,)),
        ],
        compiler_params=pltpu.CompilerParams(
            collective_id=0, has_side_effects=True, vmem_limit_bytes=48 * 1024 * 1024
        ),
    )(basis, k_tiles, m_tiles, tile_part, tile_slot, iface_rows)
    return corrections, theta.reshape(PAIRS)


def solution(mesh):
    in_specs = (
        P(None, AXIS),
        P(AXIS, None, None, None),
        P(AXIS, None, None, None),
        P(AXIS, None),
        P(AXIS, None),
        P(AXIS),
    )
    return jax.shard_map(
        shards, mesh=mesh, in_specs=in_specs, out_specs=(P(None, AXIS), P()), check_vma=False
    )
```

```python
import functools

import jax
import jax.numpy as jnp
from jax import lax
from jax.experimental import pallas as pl
from jax.experimental.pallas import tpu as pltpu
from jax.sharding import PartitionSpec as P

AXIS = "parts"
PARTS = 256
GROUP = 16
FAR = 128
PAIRS = 16
TILES = 8
BLOCKS = 5
WIDTH = 128
LOCAL = TILES * WIDTH
EXT = TILES + 6
RELAX = 0.4
MESH = pl.DeviceIdType.MESH
F32 = jnp.float32
BF16 = jnp.bfloat16
NT = (((1,), (1,)), ((), ()))
TN = (((0,), (0,)), ((), ()))


def split(x):
    hi = x.astype(BF16)
    return hi, (x - hi.astype(F32)).astype(BF16)


def mm(a, b):
    return jnp.dot(a, b, preferred_element_type=F32)


def mm_nt(a, b):
    return lax.dot_general(a, b, NT, preferred_element_type=F32)


def small(a, b, dims=(((1,), (0,)), ((), ()))):
    return lax.dot_general(
        a, b, dims, precision=lax.Precision.HIGHEST, preferred_element_type=F32
    )


def pack4(v):
    return jnp.concatenate([v[4 * i : 4 * i + 4] for i in range(4)], axis=1)


def unpack4(v):
    return jnp.concatenate([v[:, 32 * i : 32 * i + 32] for i in range(4)], axis=0)


def eliminate(gram, rows, eye):
    aug = jnp.concatenate([gram, eye], axis=1)
    for j in range(PAIRS):
        pivot = aug[j : j + 1, j : j + 1]
        d = lax.rsqrt(pivot)
        d = d * (1.5 - 0.5 * pivot * d * d)
        line = aug[j : j + 1, :] * d
        col = aug[:, j : j + 1] * d
        aug = jnp.where(rows == j, line, jnp.where(rows > j, aug - col * line, aug))
    return aug[:, PAIRS:]


def kernel(
    scale,
    basis_ref,
    k_ref,
    m_ref,
    part_hbm,
    slot_hbm,
    iface_hbm,
    out_ref,
    theta_ref,
    kbuf,
    mbuf,
    w_hi,
    w_lo,
    xt,
    dinv,
    ext16,
    ext32,
    words,
    s_hi,
    s_lo,
    pt,
    ad,
    right,
    left,
    h0out,
    h1out,
    h2out,
    h3out,
    h0in,
    h1in,
    h2in,
    h3in,
    ar_first,
    ar_big,
    ar_small,
    part_ref,
    slot_ref,
    iface_ref,
    load_sem,
    index_sem,
    x_sem,
    hs_sem,
    hr_sem,
    as_sem,
    ar_sem,
):
    me = lax.axis_index(AXIS)
    rank_a = lax.rem(me, GROUP)
    base_a = me - rank_a
    rank_b = me // GROUP
    halo_to = (
        lax.rem(me + PARTS - 1, PARTS),
        lax.rem(me + 1, PARTS),
        lax.rem(me + FAR, PARTS),
    )

    def peer_a(k):
        return base_a + lax.rem(rank_a + k, GROUP)

    def peer_b(k):
        return rank_a + GROUP * lax.rem(rank_b + k, GROUP)

    barrier = pltpu.get_barrier_semaphore()

    def greet(k, carry):
        pl.semaphore_signal(barrier, inc=1, device_id=(peer_a(k),), device_id_type=MESH)
        pl.semaphore_signal(barrier, inc=1, device_id=(peer_b(k),), device_id_type=MESH)
        return carry

    lax.fori_loop(1, GROUP, greet, 0, unroll=True)
    for device in halo_to:
        pl.semaphore_signal(barrier, inc=1, device_id=(device,), device_id_type=MESH)

    loads = []
    tables = ((part_hbm, part_ref), (slot_hbm, slot_ref), (iface_hbm, iface_ref))
    for n, (src, dst) in enumerate(tables):
        loads.append(pltpu.make_async_copy(src, dst, index_sem.at[n]))
        loads[-1].start()
    for i in range(TILES):
        loads.append(
            pltpu.make_async_copy(
                basis_ref.at[:, pl.ds(i * WIDTH, WIDTH)], xt.at[i], x_sem.at[i]
            )
        )
        loads[-1].start()
    for i in range(TILES):
        for n, (src, dst) in enumerate(((k_ref, kbuf), (m_ref, mbuf))):
            pltpu.make_async_copy(src.at[i], dst.at[i], load_sem.at[n, i]).start()

    def halo(step, out, into):
        for g, device in enumerate(halo_to):
            pltpu.make_async_remote_copy(
                src_ref=out,
                dst_ref=into.at[g],
                send_sem=hs_sem.at[step],
                recv_sem=hr_sem.at[step],
                device_id=(device,),
                device_id_type=MESH,
            ).start()

    def halo_wait(step, into):
        pltpu.make_async_copy(into, into, hr_sem.at[step]).wait()

    def spread(buf, stage, step, value):
        rank = rank_a if stage == 0 else rank_b
        peer = peer_a if stage == 0 else peer_b
        buf[rank] = value

        def send(k, carry):
            pltpu.make_async_remote_copy(
                src_ref=buf.at[rank],
                dst_ref=buf.at[rank],
                send_sem=as_sem.at[2 * step + stage],
                recv_sem=ar_sem.at[2 * step + stage],
                device_id=(peer(k),),
                device_id_type=MESH,
            ).start()
            return carry

        lax.fori_loop(1, GROUP, send, 0, unroll=True)

    def gathered(buf, stage, step):
        most = buf.at[pl.ds(0, GROUP - 1)]
        pltpu.make_async_copy(most, most, ar_sem.at[2 * step + stage]).wait()
        total = buf[0]
        for j in range(1, GROUP):
            total = total + buf[j]
        return total

    def span(i):
        return pl.ds(i * WIDTH, WIDTH)

    for copy in loads:
        copy.wait()
    columns = []
    for i in range(TILES):
        line = []
        for b in range(BLOCKS):
            part = part_ref[i, b]
            slot = slot_ref[i, b]
            where = jnp.where(
                part == halo_to[1],
                TILES,
                jnp.where(part == halo_to[0], TILES + 2, TILES + 4),
            )
            line.append(jnp.where(part == me, slot, where + slot))
        columns.append(line)
    iface = [iface_ref[0], iface_ref[1]]
    for s in range(2):
        h0out[s] = xt[iface[s]]
    pl.semaphore_wait(barrier, 33)
    halo(0, h0out, h0in)

    eye_w = lax.broadcasted_iota(jnp.int32, (WIDTH, WIDTH), 0) == lax.broadcasted_iota(
        jnp.int32, (WIDTH, WIDTH), 1
    )
    for i in range(TILES):
        hi, lo = split(xt[i])
        ext16[i, 0:16] = hi
        ext16[i, 16:32] = lo
        right[64:80, span(i)] = hi
        right[80:96, span(i)] = lo
        left[0:16, span(i)] = hi
        left[48:64, span(i)] = lo

    def prepare(i, carry):
        for n, (src, dst) in enumerate(((k_ref, kbuf), (m_ref, mbuf))):
            pltpu.make_async_copy(src.at[i], dst.at[i], load_sem.at[n, i]).wait()
            for b in range(BLOCKS):
                hi, lo = split(dst[i, b].T)
                w_hi[i, b * WIDTH : (b + 1) * WIDTH, n * WIDTH : (n + 1) * WIDTH] = hi
                w_lo[i, b * WIDTH : (b + 1) * WIDTH, n * WIDTH : (n + 1) * WIDTH] = lo
        diagonal = jnp.sum(jnp.where(eye_w, kbuf[i, 0], 0.0), axis=0, keepdims=True)
        dinv[i] = jnp.broadcast_to(1.0 / diagonal, (8, WIDTH))
        return carry

    lax.fori_loop(0, TILES, prepare, 0)
    d = [dinv[i, 0:1] for i in range(TILES)]
    for i in range(TILES):
        hi, lo = split(xt[i] * d[i])
        right[16:32, span(i)] = hi
        right[48:64, span(i)] = lo

    def apply(ext, rows, i):
        picked = jnp.concatenate([ext[columns[i][b]] for b in range(BLOCKS)], axis=1)
        high = mm(picked, w_hi[i])
        low = mm(picked[:rows], w_lo[i])
        return high[:rows] + high[rows:] + low

    halo_wait(0, h0in)
    for g in range(3):
        for s in range(2):
            hi, lo = split(h0in[g, s])
            ext16[TILES + 2 * g + s, 0:16] = hi
            ext16[TILES + 2 * g + s, 16:32] = lo
    for i in range(TILES):
        y = apply(ext16, 16, i)
        p, q = y[:, :WIDTH], y[:, WIDTH:]
        words[i, 0:16] = p * d[i]
        words[i, 16:32] = q * d[i]
        hi, lo = split(p)
        left[16:32, span(i)] = hi
        left[64:80, span(i)] = lo
        hi, lo = split(q)
        left[32:48, span(i)] = hi
        left[80:96, span(i)] = lo
        right[0:16, span(i)] = hi
        right[32:48, span(i)] = lo
    for s in range(2):
        h1out[s] = words[iface[s], 0:32]
    halo(1, h1out, h1in)

    gram = mm_nt(left[0:96], right[...])
    gram = gram[0:48] + gram[48:96]
    with_qx = gram[:, 0:32] + gram[:, 32:64]
    with_x = gram[:, 64:80] + gram[:, 80:96]
    alone = jnp.concatenate([with_x[0:16], jnp.zeros((16, 16), F32)], axis=1)
    payload = jnp.stack([pack4(with_qx[16:32]), pack4(with_qx[32:48]), pack4(alone)])
    spread(ar_first.at[0], 0, 0, payload)

    for i in range(TILES):
        hi, lo = split(words[i, 0:32])
        ext32[i, 0:32] = hi
        ext32[i, 32:64] = lo
        s_hi[i, 0:32] = hi
        s_lo[i, 0:32] = lo
    halo_wait(1, h1in)
    for g in range(3):
        for s in range(2):
            hi, lo = split(h1in[g, s])
            t = TILES + 2 * g + s
            ext32[t, 0:32] = hi
            ext32[t, 32:64] = lo
            s_hi[t, 0:32] = hi
            s_lo[t, 0:32] = lo

    for i in range(TILES):
        y = apply(ext32, 32, i)
        stiff, mass = y[:, :WIDTH], y[:, WIDTH:]
        hi, lo = split(stiff)
        left[0:32, span(i)] = hi
        left[64:96, span(i)] = lo
        hi, lo = split(mass)
        left[32:64, span(i)] = hi
        left[96:128, span(i)] = lo
        stiff, mass = stiff * d[i], mass * d[i]
        words[i, 32:48] = stiff[16:32]
        words[i, 48:64] = mass[16:32]
        words[i, 64:80] = stiff[0:16]
        words[i, 80:96] = mass[0:16]
    for s in range(2):
        h2out[s] = words[iface[s], 32:96]
    halo(2, h2out, h2in)
    spread(ar_first.at[1], 1, 0, gathered(ar_first.at[0], 0, 0))
    gram = mm_nt(left[...], right[0:64])
    gram = gram[0:64] + gram[64:128]
    gram = gram[:, 0:32] + gram[:, 32:64]
    payload = jnp.concatenate([gram[16 * r : 16 * r + 16] for r in range(4)], axis=1)
    spread(ar_big.at[0], 0, 1, payload)
    for i in range(TILES):
        hi, lo = split(words[i, 32:96])
        s_hi[i, 32:96] = hi
        s_lo[i, 32:96] = lo

    total = gathered(ar_first.at[1], 1, 0) * scale
    g_p, g_q, g_xx = unpack4(total[0]), unpack4(total[1]), unpack4(total[2])[:, 0:16]
    g_pq, g_px = g_p[:, 0:16], g_p[:, 16:32]
    g_qq, g_qx = g_q[:, 0:16], g_q[:, 16:32]
    row_no = lax.broadcasted_iota(jnp.int32, (PAIRS, 2 * PAIRS), 0)
    eye_b = lax.broadcasted_iota(jnp.int32, (PAIRS, PAIRS), 0) == lax.broadcasted_iota(
        jnp.int32, (PAIRS, PAIRS), 1
    )
    eye = jnp.where(eye_b, 1.0, 0.0).astype(F32)
    inv_v = eliminate(g_xx, row_no, eye)
    inv_m = eliminate(g_qq, row_no, eye)
    projected = small(inv_m, g_pq, NT)
    diag_v = jnp.sum(jnp.where(eye_b, inv_v, 0.0), axis=1, keepdims=True)
    diag_m = jnp.sum(jnp.where(eye_b, inv_m, 0.0), axis=1, keepdims=True)
    theta = jnp.sum(projected * inv_v, axis=1, keepdims=True) * diag_m / diag_v
    theta_ref[...] = jnp.sum(jnp.where(eye_b, theta, 0.0), axis=0, keepdims=True)
    wide = jnp.broadcast_to(theta, (PAIRS, WIDTH))
    gram_v = small(inv_v, inv_v, TN)
    gram_m = small(inv_m, inv_m, TN)
    start_p = -RELAX * inv_v
    start_q = RELAX * theta * inv_v
    start_x = small(start_p, g_px) + small(start_q, g_qx)
    r = small(start_x, gram_v)
    r_pq = small(r, g_pq)
    coef = jnp.concatenate(
        [
            2.0 * start_p + RELAX * r,
            2.0 * start_q,
            -RELAX * start_q,
            RELAX * theta * start_q,
            -RELAX * start_p,
            RELAX * theta * start_p,
        ],
        axis=1,
    )
    spread(ar_big.at[1], 1, 1, gathered(ar_big.at[0], 0, 1))
    halo_wait(2, h2in)
    for g in range(3):
        for s in range(2):
            hi, lo = split(h2in[g, s])
            t = TILES + 2 * g + s
            s_hi[t, 32:96] = hi
            s_lo[t, 32:96] = lo

    def combine(coef, rows, t):
        hi, lo = split(coef)
        both = jnp.concatenate([hi, lo], axis=0)
        first = mm(both, s_hi[t, 0:rows])
        second = mm(hi, s_lo[t, 0:rows])
        return first[0:16] + first[16:32] + second

    for t in range(EXT):
        p = combine(coef, 96, t)
        pt[t] = p
        hi, lo = split(p)
        ext16[t, 0:16] = hi
        ext16[t, 16:32] = lo

    def forward(step):
        got = gathered(ar_small.at[2 * step - 2], 0, step + 1)
        spread(ar_small.at[2 * step - 1], 1, step + 1, got)

    def residual(step, last):
        for i in range(TILES):
            y = apply(ext16, 16, i)
            image = y[:, :WIDTH] - wide * y[:, WIDTH:]
            hi, lo = split(image)
            left[0:16, span(i)] = hi
            left[16:32, span(i)] = lo
            ad[i] = image * d[i]
        if not last:
            out = h3out.at[step - 1]
            for s in range(2):
                out[s] = ad[iface[s]]
            halo(step + 2, out, h3in.at[step - 1])
        if step == 2:
            forward(1)
        gram = mm_nt(left[0:32], right[0:64])
        gram = gram[0:16] + gram[16:32]
        gram = gram[:, 0:32] + gram[:, 32:64]
        spread(ar_small.at[2 * step - 2], 0, step + 1, pack4(gram))

    residual(1, False)

    total = gathered(ar_big.at[1], 1, 1) * scale
    kq, mq = total[:, 32:64], total[:, 96:128]
    kp, mp = total[:, 0:32], total[:, 64:96]
    image = (small(start_p, kp) + small(start_q, kq)) - theta * (
        small(start_p, mp) + small(start_q, mq)
    )
    p_x = 2.0 * start_x - RELAX * image[:, 16:32] + RELAX * small(r, g_px)

    for step in (1, 2, 3):
        m = small(image[:, 0:16] - r_pq, gram_m)
        c_x = p_x + RELAX * small(m, g_qx)
        r = small(c_x, gram_v)
        m_image = RELAX * (small(m, kq) - theta * small(m, mq))
        coef = jnp.concatenate(
            [
                start_p + RELAX * r,
                start_q + RELAX * m,
                -RELAX * RELAX * m,
                RELAX * RELAX * theta * m,
            ],
            axis=1,
        )
        if step < 3:
            for t in range(TILES):
                p = pt[t] - RELAX * ad[t] + combine(coef, 64, t)
                pt[t] = p
                hi, lo = split(p)
                ext16[t, 0:16] = hi
                ext16[t, 16:32] = lo
            for t in range(TILES, EXT):
                pt[t] = pt[t] + combine(coef, 64, t)
            if step == 2:
                forward(2)
            halo_wait(step + 2, h3in.at[step - 1])
            for g in range(3):
                for s in range(2):
                    t = TILES + 2 * g + s
                    p = pt[t] - RELAX * h3in[step - 1, g, s]
                    pt[t] = p
                    hi, lo = split(p)
                    ext16[t, 0:16] = hi
                    ext16[t, 16:32] = lo
            residual(step + 1, step == 2)
        else:
            forward(3)
            for t in range(TILES):
                pt[t] = pt[t] - RELAX * ad[t] + combine(coef, 64, t)
        r_px = small(r, g_px)
        r_pq = small(r, g_pq)
        total = unpack4(gathered(ar_small.at[2 * step - 1], 1, step + 1)) * scale
        image = total + m_image
        p_x = c_x + start_x - RELAX * image[:, 16:32] + RELAX * r_px

    m = small(image[:, 0:16] - r_pq, gram_m)
    c_x = p_x + RELAX * small(m, g_qx)
    r = small(c_x, gram_v)
    q_hi, q_lo = split(RELAX * m)
    x_hi, x_lo = split(-r)
    lead = jnp.concatenate([q_hi, x_hi], axis=1)
    rest = jnp.concatenate([q_lo, x_lo], axis=1)
    for t in range(TILES):
        hi = jnp.concatenate([s_hi[t, 16:32], right[64:80, span(t)]], axis=0)
        lo = jnp.concatenate([s_lo[t, 16:32], right[80:96, span(t)]], axis=0)
        out_ref[:, span(t)] = pt[t] + (mm(lead, hi) + mm(rest, hi) + mm(lead, lo))

    for step, out in enumerate((h0out, h1out, h2out, h3out.at[0], h3out.at[1])):
        for g in range(3):
            pltpu.make_async_copy(out, out, hs_sem.at[step]).wait()
    for step in range(5):
        for stage in range(2):
            buf = (ar_first, ar_big, ar_small, ar_small, ar_small)[step]
            buf = buf.at[max(2 * step - 4, 0) + stage]
            most = buf.at[pl.ds(0, GROUP - 1)]
            pltpu.make_async_copy(most, most, as_sem.at[2 * step + stage]).wait()


def shards(basis, k_tiles, m_tiles, tile_part, tile_slot, iface_rows):
    rows = basis.shape[1] * lax.axis_size(AXIS)
    vmem = pltpu.VMEM
    corrections, theta = pl.pallas_call(
        functools.partial(kernel, 1.0 / rows),
        out_shape=(
            jax.ShapeDtypeStruct((PAIRS, LOCAL), F32),
            jax.ShapeDtypeStruct((1, PAIRS), F32),
        ),
        in_specs=[pl.BlockSpec(memory_space=pltpu.HBM)] * 6,
        out_specs=(pl.BlockSpec(memory_space=vmem), pl.BlockSpec(memory_space=vmem)),
        scratch_shapes=[
            vmem((TILES, BLOCKS, WIDTH, WIDTH), F32),
            vmem((TILES, BLOCKS, WIDTH, WIDTH), F32),
            vmem((TILES, BLOCKS * WIDTH, 2 * WIDTH), BF16),
            vmem((TILES, BLOCKS * WIDTH, 2 * WIDTH), BF16),
            vmem((TILES, 16, WIDTH), F32),
            vmem((TILES, 8, WIDTH), F32),
            vmem((EXT, 32, WIDTH), BF16),
            vmem((EXT, 64, WIDTH), BF16),
            vmem((TILES, 96, WIDTH), F32),
            vmem((EXT, 96, WIDTH), BF16),
            vmem((EXT, 96, WIDTH), BF16),
            vmem((EXT, 16, WIDTH), F32),
            vmem((TILES, 16, WIDTH), F32),
            vmem((96, LOCAL), BF16),
            vmem((128, LOCAL), BF16),
            vmem((2, 16, WIDTH), F32),
            vmem((2, 32, WIDTH), F32),
            vmem((2, 64, WIDTH), F32),
            vmem((2, 2, 16, WIDTH), F32),
            vmem((3, 2, 16, WIDTH), F32),
            vmem((3, 2, 32, WIDTH), F32),
            vmem((3, 2, 64, WIDTH), F32),
            vmem((2, 3, 2, 16, WIDTH), F32),
            vmem((2, GROUP, 3, 4, WIDTH), F32),
            vmem((2, GROUP, 16, WIDTH), F32),
            vmem((6, GROUP, 4, WIDTH), F32),
            pltpu.SMEM((TILES, BLOCKS), jnp.int32),
            pltpu.SMEM((TILES, BLOCKS), jnp.int32),
            pltpu.SMEM((2,), jnp.int32),
            pltpu.SemaphoreType.DMA((2, TILES)),
            pltpu.SemaphoreType.DMA((3,)),
            pltpu.SemaphoreType.DMA((TILES,)),
            pltpu.SemaphoreType.DMA((5,)),
            pltpu.SemaphoreType.DMA((5,)),
            pltpu.SemaphoreType.DMA((10,)),
            pltpu.SemaphoreType.DMA((10,)),
        ],
        compiler_params=pltpu.CompilerParams(
            collective_id=0, has_side_effects=True, vmem_limit_bytes=60 * 1024 * 1024
        ),
    )(basis, k_tiles, m_tiles, tile_part, tile_slot, iface_rows)
    return corrections, theta.reshape(PAIRS)


def solution(mesh):
    in_specs = (
        P(None, AXIS),
        P(AXIS, None, None, None),
        P(AXIS, None, None, None),
        P(AXIS, None),
        P(AXIS, None),
        P(AXIS),
    )
    return jax.shard_map(
        shards, mesh=mesh, in_specs=in_specs, out_specs=(P(None, AXIS), P()), check_vma=False
    )
```

```python
import functools

import jax
import jax.numpy as jnp
from jax import lax
from jax.experimental import pallas as pl
from jax.experimental.pallas import tpu as pltpu
from jax.sharding import PartitionSpec as P

AXIS = "parts"
PARTS = 256
GROUP = 16
FAR = 128
PAIRS = 16
TILES = 8
BLOCKS = 5
WIDTH = 128
LOCAL = TILES * WIDTH
EXT = TILES + 6
RELAX = 0.4
MESH = pl.DeviceIdType.MESH
F32 = jnp.float32
BF16 = jnp.bfloat16
NT = (((1,), (1,)), ((), ()))
TN = (((0,), (0,)), ((), ()))


def split(x):
    hi = x.astype(BF16)
    return hi, (x - hi.astype(F32)).astype(BF16)


def mm(a, b):
    return jnp.dot(a, b, preferred_element_type=F32)


def mm_nt(a, b):
    return lax.dot_general(a, b, NT, preferred_element_type=F32)


def small(a, b, dims=(((1,), (0,)), ((), ()))):
    return lax.dot_general(
        a, b, dims, precision=lax.Precision.HIGHEST, preferred_element_type=F32
    )


def pack4(v):
    return jnp.concatenate([v[4 * i : 4 * i + 4] for i in range(4)], axis=1)


def unpack4(v):
    return jnp.concatenate([v[:, 32 * i : 32 * i + 32] for i in range(4)], axis=0)


def eliminate(gram, rows, eye):
    aug = jnp.concatenate([gram, eye], axis=1)
    for j in range(PAIRS):
        pivot = aug[j : j + 1, j : j + 1]
        d = lax.rsqrt(pivot)
        d = d * (1.5 - 0.5 * pivot * d * d)
        line = aug[j : j + 1, :] * d
        col = aug[:, j : j + 1] * d
        aug = jnp.where(rows == j, line, jnp.where(rows > j, aug - col * line, aug))
    return aug[:, PAIRS:]


def kernel(
    scale,
    basis_ref,
    k_ref,
    m_ref,
    part_hbm,
    slot_hbm,
    iface_hbm,
    out_ref,
    theta_ref,
    kbuf,
    mbuf,
    w_hi,
    w_lo,
    xt,
    dinv,
    ext16,
    ext32,
    words,
    s_hi,
    s_lo,
    pt,
    ad,
    right,
    left,
    h0out,
    h1out,
    h2out,
    h3out,
    h0in,
    h1in,
    h2in,
    h3in,
    ar_first,
    ar_big,
    ar_small,
    ar_third,
    ar_extra,
    back,
    adj,
    zin,
    right2,
    part_ref,
    slot_ref,
    iface_ref,
    load_sem,
    index_sem,
    x_sem,
    hs_sem,
    hr_sem,
    as_sem,
    ar_sem,
):
    me = lax.axis_index(AXIS)
    rank_a = lax.rem(me, GROUP)
    base_a = me - rank_a
    rank_b = me // GROUP
    halo_to = (
        lax.rem(me + PARTS - 1, PARTS),
        lax.rem(me + 1, PARTS),
        lax.rem(me + FAR, PARTS),
    )

    def peer_a(k):
        return base_a + lax.rem(rank_a + k, GROUP)

    def peer_b(k):
        return rank_a + GROUP * lax.rem(rank_b + k, GROUP)

    barrier = pltpu.get_barrier_semaphore()

    def greet(k, carry):
        pl.semaphore_signal(barrier, inc=1, device_id=(peer_a(k),), device_id_type=MESH)
        pl.semaphore_signal(barrier, inc=1, device_id=(peer_b(k),), device_id_type=MESH)
        return carry

    lax.fori_loop(1, GROUP, greet, 0, unroll=True)
    for device in halo_to:
        pl.semaphore_signal(barrier, inc=1, device_id=(device,), device_id_type=MESH)

    loads = []
    tables = ((part_hbm, part_ref), (slot_hbm, slot_ref), (iface_hbm, iface_ref))
    for n, (src, dst) in enumerate(tables):
        loads.append(pltpu.make_async_copy(src, dst, index_sem.at[n]))
        loads[-1].start()
    for i in range(TILES):
        loads.append(
            pltpu.make_async_copy(
                basis_ref.at[:, pl.ds(i * WIDTH, WIDTH)], xt.at[i], x_sem.at[i]
            )
        )
        loads[-1].start()
    for i in range(TILES):
        for n, (src, dst) in enumerate(((k_ref, kbuf), (m_ref, mbuf))):
            pltpu.make_async_copy(src.at[i], dst.at[i], load_sem.at[n, i]).start()

    def halo(step, out, into):
        for g, device in enumerate(halo_to):
            pltpu.make_async_remote_copy(
                src_ref=out,
                dst_ref=into.at[g],
                send_sem=hs_sem.at[step],
                recv_sem=hr_sem.at[step],
                device_id=(device,),
                device_id_type=MESH,
            ).start()

    def halo_wait(step, into):
        pltpu.make_async_copy(into, into, hr_sem.at[step]).wait()

    def spread(buf, stage, step, value):
        rank = rank_a if stage == 0 else rank_b
        peer = peer_a if stage == 0 else peer_b
        buf[rank] = value

        def send(k, carry):
            pltpu.make_async_remote_copy(
                src_ref=buf.at[rank],
                dst_ref=buf.at[rank],
                send_sem=as_sem.at[2 * step + stage],
                recv_sem=ar_sem.at[2 * step + stage],
                device_id=(peer(k),),
                device_id_type=MESH,
            ).start()
            return carry

        lax.fori_loop(1, GROUP, send, 0, unroll=True)

    def gathered(buf, stage, step):
        most = buf.at[pl.ds(0, GROUP - 1)]
        pltpu.make_async_copy(most, most, ar_sem.at[2 * step + stage]).wait()
        total = buf[0]
        for j in range(1, GROUP):
            total = total + buf[j]
        return total

    def span(i):
        return pl.ds(i * WIDTH, WIDTH)

    for copy in loads:
        copy.wait()
    columns = []
    for i in range(TILES):
        line = []
        for b in range(BLOCKS):
            part = part_ref[i, b]
            slot = slot_ref[i, b]
            where = jnp.where(
                part == halo_to[1],
                TILES,
                jnp.where(part == halo_to[0], TILES + 2, TILES + 4),
            )
            line.append(jnp.where(part == me, slot, where + slot))
        columns.append(line)
    iface = [iface_ref[0], iface_ref[1]]
    for s in range(2):
        h0out[s] = xt[iface[s]]
    pl.semaphore_wait(barrier, 33)
    halo(0, h0out, h0in)

    eye_w = lax.broadcasted_iota(jnp.int32, (WIDTH, WIDTH), 0) == lax.broadcasted_iota(
        jnp.int32, (WIDTH, WIDTH), 1
    )
    for i in range(TILES):
        hi, lo = split(xt[i])
        ext16[i, 0:16] = hi
        ext16[i, 16:32] = lo
        right[64:80, span(i)] = hi
        right[80:96, span(i)] = lo
        left[0:16, span(i)] = hi
        left[48:64, span(i)] = lo

    def prepare(i, carry):
        for n, (src, dst) in enumerate(((k_ref, kbuf), (m_ref, mbuf))):
            pltpu.make_async_copy(src.at[i], dst.at[i], load_sem.at[n, i]).wait()
            for b in range(BLOCKS):
                hi, lo = split(dst[i, b].T)
                w_hi[i, b * WIDTH : (b + 1) * WIDTH, n * WIDTH : (n + 1) * WIDTH] = hi
                w_lo[i, b * WIDTH : (b + 1) * WIDTH, n * WIDTH : (n + 1) * WIDTH] = lo
        diagonal = jnp.sum(jnp.where(eye_w, kbuf[i, 0], 0.0), axis=0, keepdims=True)
        dinv[i] = jnp.broadcast_to(1.0 / diagonal, (8, WIDTH))
        return carry

    lax.fori_loop(0, TILES, prepare, 0)
    d = [dinv[i, 0:1] for i in range(TILES)]
    for i in range(TILES):
        hi, lo = split(xt[i] * d[i])
        right[16:32, span(i)] = hi
        right[48:64, span(i)] = lo

    def apply(ext, rows, i):
        picked = jnp.concatenate([ext[columns[i][b]] for b in range(BLOCKS)], axis=1)
        high = mm(picked, w_hi[i])
        low = mm(picked[:rows], w_lo[i])
        return high[:rows] + high[rows:] + low

    halo_wait(0, h0in)
    for g in range(3):
        for s in range(2):
            hi, lo = split(h0in[g, s])
            ext16[TILES + 2 * g + s, 0:16] = hi
            ext16[TILES + 2 * g + s, 16:32] = lo
    for i in range(TILES):
        y = apply(ext16, 16, i)
        p, q = y[:, :WIDTH], y[:, WIDTH:]
        words[i, 0:16] = p * d[i]
        words[i, 16:32] = q * d[i]
        hi, lo = split(p)
        left[16:32, span(i)] = hi
        left[64:80, span(i)] = lo
        hi, lo = split(q)
        left[32:48, span(i)] = hi
        left[80:96, span(i)] = lo
        right[0:16, span(i)] = hi
        right[32:48, span(i)] = lo
    for s in range(2):
        h1out[s] = words[iface[s], 0:32]
    halo(1, h1out, h1in)

    gram = mm_nt(left[0:96], right[...])
    gram = gram[0:48] + gram[48:96]
    with_qx = gram[:, 0:32] + gram[:, 32:64]
    with_x = gram[:, 64:80] + gram[:, 80:96]
    alone = jnp.concatenate([with_x[0:16], jnp.zeros((16, 16), F32)], axis=1)
    payload = jnp.stack([pack4(with_qx[16:32]), pack4(with_qx[32:48]), pack4(alone)])
    spread(ar_first.at[0], 0, 0, payload)

    for i in range(TILES):
        hi, lo = split(words[i, 0:32])
        ext32[i, 0:32] = hi
        ext32[i, 32:64] = lo
        s_hi[i, 0:32] = hi
        s_lo[i, 0:32] = lo
    for i in range(TILES):
        hi, lo = right[0:32, span(i)], right[32:64, span(i)]
        none = jnp.zeros((32, WIDTH), BF16)
        hi = jnp.concatenate(
            [jnp.concatenate([hi, none], axis=1), jnp.concatenate([none, hi], axis=1)], axis=0
        )
        lo = jnp.concatenate(
            [jnp.concatenate([lo, none], axis=1), jnp.concatenate([none, lo], axis=1)], axis=0
        )
        high = mm_nt(jnp.concatenate([hi, lo], axis=0), w_hi[i])
        share = high[0:64] + high[64:128] + mm_nt(hi, w_lo[i])
        for b in range(BLOCKS):
            back[i, b] = share[:, b * WIDTH : (b + 1) * WIDTH]

    def collect(j, total):
        for i in range(TILES):
            for b in range(1, BLOCKS):
                total = total + jnp.where(columns[i][b] == j, back[i, b], 0.0)
        adj[j] = total

    def collect_remote(j, carry):
        collect(j, jnp.zeros((64, WIDTH), F32))
        return carry

    def collect_local(j, carry):
        collect(j, back[j, 0])
        return carry

    lax.fori_loop(TILES, EXT, collect_remote, 0)
    halo_wait(1, h1in)
    for g in range(3):
        for s in range(2):
            hi, lo = split(h1in[g, s])
            t = TILES + 2 * g + s
            ext32[t, 0:32] = hi
            ext32[t, 32:64] = lo
            s_hi[t, 0:32] = hi
            s_lo[t, 0:32] = lo

    for i in range(TILES):
        y = apply(ext32, 32, i)
        stiff, mass = y[:, :WIDTH], y[:, WIDTH:]
        hi, lo = split(stiff)
        left[0:32, span(i)] = hi
        left[64:96, span(i)] = lo
        hi, lo = split(mass)
        left[32:64, span(i)] = hi
        left[96:128, span(i)] = lo
        stiff, mass = stiff * d[i], mass * d[i]
        words[i, 32:48] = stiff[16:32]
        words[i, 48:64] = mass[16:32]
        words[i, 64:80] = stiff[0:16]
        words[i, 80:96] = mass[0:16]
    for s in range(2):
        h2out[s] = words[iface[s], 32:96]
    halo(2, h2out, h2in)
    spread(ar_first.at[1], 1, 0, gathered(ar_first.at[0], 0, 0))
    gram = mm_nt(left[...], right[0:64])
    gram = gram[0:64] + gram[64:128]
    gram = gram[:, 0:32] + gram[:, 32:64]
    payload = jnp.concatenate([gram[16 * r : 16 * r + 16] for r in range(4)], axis=1)
    spread(ar_big.at[0], 0, 1, payload)
    for g, device in enumerate((halo_to[1], halo_to[0], halo_to[2])):
        pltpu.make_async_remote_copy(
            src_ref=adj.at[pl.ds(TILES + 2 * g, 2)],
            dst_ref=zin.at[g],
            send_sem=hs_sem.at[5],
            recv_sem=hr_sem.at[5],
            device_id=(device,),
            device_id_type=MESH,
        ).start()
    for i in range(TILES):
        hi, lo = split(words[i, 32:96])
        s_hi[i, 32:96] = hi
        s_lo[i, 32:96] = lo
    lax.fori_loop(0, TILES, collect_local, 0)

    total = gathered(ar_first.at[1], 1, 0) * scale
    g_p, g_q, g_xx = unpack4(total[0]), unpack4(total[1]), unpack4(total[2])[:, 0:16]
    g_pq, g_px = g_p[:, 0:16], g_p[:, 16:32]
    g_qq, g_qx = g_q[:, 0:16], g_q[:, 16:32]
    row_no = lax.broadcasted_iota(jnp.int32, (PAIRS, 2 * PAIRS), 0)
    eye_b = lax.broadcasted_iota(jnp.int32, (PAIRS, PAIRS), 0) == lax.broadcasted_iota(
        jnp.int32, (PAIRS, PAIRS), 1
    )
    eye = jnp.where(eye_b, 1.0, 0.0).astype(F32)
    inv_v = eliminate(g_xx, row_no, eye)
    inv_m = eliminate(g_qq, row_no, eye)
    projected = small(inv_m, g_pq, NT)
    diag_v = jnp.sum(jnp.where(eye_b, inv_v, 0.0), axis=1, keepdims=True)
    diag_m = jnp.sum(jnp.where(eye_b, inv_m, 0.0), axis=1, keepdims=True)
    theta = jnp.sum(projected * inv_v, axis=1, keepdims=True) * diag_m / diag_v
    theta_ref[...] = jnp.sum(jnp.where(eye_b, theta, 0.0), axis=0, keepdims=True)
    wide = jnp.broadcast_to(theta, (PAIRS, WIDTH))
    gram_v = small(inv_v, inv_v, TN)
    gram_m = small(inv_m, inv_m, TN)
    start_p = -RELAX * inv_v
    start_q = RELAX * theta * inv_v
    start_x = small(start_p, g_px) + small(start_q, g_qx)
    r = small(start_x, gram_v)
    r_pq = small(r, g_pq)
    coef = jnp.concatenate(
        [
            2.0 * start_p + RELAX * r,
            2.0 * start_q,
            -RELAX * start_q,
            RELAX * theta * start_q,
            -RELAX * start_p,
            RELAX * theta * start_p,
        ],
        axis=1,
    )
    spread(ar_big.at[1], 1, 1, gathered(ar_big.at[0], 0, 1))
    halo_wait(2, h2in)
    for g in range(3):
        for s in range(2):
            hi, lo = split(h2in[g, s])
            t = TILES + 2 * g + s
            s_hi[t, 32:96] = hi
            s_lo[t, 32:96] = lo

    def combine(coef, rows, t):
        hi, lo = split(coef)
        both = jnp.concatenate([hi, lo], axis=0)
        first = mm(both, s_hi[t, 0:rows])
        second = mm(hi, s_lo[t, 0:rows])
        return first[0:16] + first[16:32] + second

    for t in range(EXT):
        p = combine(coef, 96, t)
        pt[t] = p
        hi, lo = split(p)
        ext16[t, 0:16] = hi
        ext16[t, 16:32] = lo

    def residual(step):
        for i in range(TILES):
            y = apply(ext16, 16, i)
            image = y[:, :WIDTH] - wide * y[:, WIDTH:]
            moved = image * d[i]
            ad[i] = moved
            if step < 3:
                hi, lo = split(image)
                left[0:16, span(i)] = hi
                left[16:32, span(i)] = lo
            if step == 2:
                hi, lo = split(moved)
                left[32:48, span(i)] = hi
                left[48:64, span(i)] = lo
        if step < 3:
            out = h3out.at[step - 1]
            for s in range(2):
                out[s] = ad[iface[s]]
            halo(step + 2, out, h3in.at[step - 1])

    def with_qxd(rows):
        gram = mm_nt(left[0 : 2 * rows], right[0:64])
        gram = gram[0:rows] + gram[rows : 2 * rows]
        return gram[:, 0:32] + gram[:, 32:64]

    def with_back(both, rows):
        gram = mm_nt(both, right2[...])
        gram = gram[0:rows] + gram[rows : 2 * rows]
        return gram[:, 0:64] + gram[:, 64:128]

    residual(1)
    gram = with_qxd(16)
    spread(ar_small.at[0], 0, 2, pack4(gram))

    pltpu.make_async_copy(zin, zin, hr_sem.at[5]).wait()
    for j in range(TILES):
        total = adj[j]
        for s in range(2):
            for g in range(3):
                total = total + jnp.where(iface[s] == j, zin[g, s], 0.0)
        hi, lo = split(total)
        right2[0:64, span(j)] = hi
        right2[64:128, span(j)] = lo
    both = jnp.concatenate(
        [
            jnp.concatenate([s_hi[t, 32:64] for t in range(TILES)], axis=1),
            jnp.concatenate([s_lo[t, 32:64] for t in range(TILES)], axis=1),
        ],
        axis=0,
    )
    gram = with_back(both, 32)
    spread(ar_extra.at[0], 0, 4, jnp.concatenate([gram[0:16], gram[16:32]], axis=1))

    total = gathered(ar_big.at[1], 1, 1) * scale
    kq, mq = total[:, 32:64], total[:, 96:128]
    kp, mp = total[:, 0:32], total[:, 64:96]
    image = (small(start_p, kp) + small(start_q, kq)) - theta * (
        small(start_p, mp) + small(start_q, mq)
    )
    p_x = 2.0 * start_x - RELAX * image[:, 16:32] + RELAX * small(r, g_px)

    def advance(image, r_pq, p_x):
        m = small(image[:, 0:16] - r_pq, gram_m)
        c_x = p_x + RELAX * small(m, g_qx)
        return m, c_x, small(c_x, gram_v)

    def coefficients(m, r):
        parts = [
            start_p + RELAX * r,
            start_q + RELAX * m,
            -RELAX * RELAX * m,
            RELAX * RELAX * theta * m,
        ]
        return jnp.concatenate(parts, axis=1)

    def image_of(m):
        return RELAX * (small(m, kq) - theta * small(m, mq))

    for step in (1, 2):
        m, c_x, r = advance(image, r_pq, p_x)
        m_image = image_of(m)
        coef = coefficients(m, r)
        for t in range(TILES):
            p = pt[t] - RELAX * ad[t] + combine(coef, 64, t)
            pt[t] = p
            hi, lo = split(p)
            ext16[t, 0:16] = hi
            ext16[t, 16:32] = lo
        for t in range(TILES, EXT):
            pt[t] = pt[t] + combine(coef, 64, t)
        if step == 2:
            spread(ar_third.at[1], 1, 3, gathered(ar_third.at[0], 0, 3))
        halo_wait(step + 2, h3in.at[step - 1])
        for g in range(3):
            for s in range(2):
                t = TILES + 2 * g + s
                p = pt[t] - RELAX * h3in[step - 1, g, s]
                pt[t] = p
                hi, lo = split(p)
                ext16[t, 0:16] = hi
                ext16[t, 16:32] = lo
        residual(step + 1)
        r_px = small(r, g_px)
        r_pq = small(r, g_pq)
        if step == 1:
            spread(ar_small.at[1], 1, 2, gathered(ar_small.at[0], 0, 2))
            gram = with_qxd(16)
            gram_b = with_back(left[32:64], 16)
            gram_b = gram_b[:, 0:32] - theta * gram_b[:, 32:64]
            spread(ar_third.at[0], 0, 3, jnp.stack([pack4(gram), pack4(gram_b)]))
            spread(ar_extra.at[1], 1, 4, gathered(ar_extra.at[0], 0, 4))
            image = unpack4(gathered(ar_small.at[1], 1, 2)) * scale + m_image
            p_x = c_x + start_x - RELAX * image[:, 16:32] + RELAX * r_px

    extra = gathered(ar_extra.at[1], 1, 4) * scale
    stiff = jnp.concatenate([kp, kq, extra[:, 0:32], extra[:, 64:96]], axis=0)
    mass = jnp.concatenate([mp, mq, extra[:, 32:64], extra[:, 96:128]], axis=0)
    known = small(coef, stiff) - theta * small(coef, mass)
    total = gathered(ar_third.at[1], 1, 3) * scale
    image = unpack4(total[0])
    known = known + image - RELAX * unpack4(total[1])
    image = image + m_image
    p_x = c_x + start_x - RELAX * image[:, 16:32] + RELAX * r_px
    m, c_x, r = advance(image, r_pq, p_x)
    coef = coefficients(m, r)
    image = known + image_of(m)
    r_pq = small(r, g_pq)
    p_x = c_x + start_x - RELAX * image[:, 16:32] + RELAX * small(r, g_px)
    for t in range(TILES):
        pt[t] = pt[t] - RELAX * ad[t] + combine(coef, 64, t)

    m, c_x, r = advance(image, r_pq, p_x)
    q_hi, q_lo = split(RELAX * m)
    x_hi, x_lo = split(-r)
    lead = jnp.concatenate([q_hi, x_hi], axis=1)
    rest = jnp.concatenate([q_lo, x_lo], axis=1)
    for t in range(TILES):
        hi = jnp.concatenate([s_hi[t, 16:32], right[64:80, span(t)]], axis=0)
        lo = jnp.concatenate([s_lo[t, 16:32], right[80:96, span(t)]], axis=0)
        out_ref[:, span(t)] = pt[t] + (mm(lead, hi) + mm(rest, hi) + mm(lead, lo))

    for step, out in enumerate((h0out, h1out, h2out, h3out.at[0], h3out.at[1])):
        for g in range(3):
            pltpu.make_async_copy(out, out, hs_sem.at[step]).wait()
    sent = adj.at[pl.ds(TILES, 6)]
    pltpu.make_async_copy(sent, sent, hs_sem.at[5]).wait()
    for step, buf in enumerate((ar_first, ar_big, ar_small, ar_third, ar_extra)):
        for stage in range(2):
            most = buf.at[stage, pl.ds(0, GROUP - 1)]
            pltpu.make_async_copy(most, most, as_sem.at[2 * step + stage]).wait()


def shards(basis, k_tiles, m_tiles, tile_part, tile_slot, iface_rows):
    rows = basis.shape[1] * lax.axis_size(AXIS)
    vmem = pltpu.VMEM
    corrections, theta = pl.pallas_call(
        functools.partial(kernel, 1.0 / rows),
        out_shape=(
            jax.ShapeDtypeStruct((PAIRS, LOCAL), F32),
            jax.ShapeDtypeStruct((1, PAIRS), F32),
        ),
        in_specs=[pl.BlockSpec(memory_space=pltpu.HBM)] * 6,
        out_specs=(pl.BlockSpec(memory_space=vmem), pl.BlockSpec(memory_space=vmem)),
        scratch_shapes=[
            vmem((TILES, BLOCKS, WIDTH, WIDTH), F32),
            vmem((TILES, BLOCKS, WIDTH, WIDTH), F32),
            vmem((TILES, BLOCKS * WIDTH, 2 * WIDTH), BF16),
            vmem((TILES, BLOCKS * WIDTH, 2 * WIDTH), BF16),
            vmem((TILES, 16, WIDTH), F32),
            vmem((TILES, 8, WIDTH), F32),
            vmem((EXT, 32, WIDTH), BF16),
            vmem((EXT, 64, WIDTH), BF16),
            vmem((TILES, 96, WIDTH), F32),
            vmem((EXT, 96, WIDTH), BF16),
            vmem((EXT, 96, WIDTH), BF16),
            vmem((EXT, 16, WIDTH), F32),
            vmem((TILES, 16, WIDTH), F32),
            vmem((96, LOCAL), BF16),
            vmem((128, LOCAL), BF16),
            vmem((2, 16, WIDTH), F32),
            vmem((2, 32, WIDTH), F32),
            vmem((2, 64, WIDTH), F32),
            vmem((2, 2, 16, WIDTH), F32),
            vmem((3, 2, 16, WIDTH), F32),
            vmem((3, 2, 32, WIDTH), F32),
            vmem((3, 2, 64, WIDTH), F32),
            vmem((2, 3, 2, 16, WIDTH), F32),
            vmem((2, GROUP, 3, 4, WIDTH), F32),
            vmem((2, GROUP, 16, WIDTH), F32),
            vmem((2, GROUP, 4, WIDTH), F32),
            vmem((2, GROUP, 2, 4, WIDTH), F32),
            vmem((2, GROUP, 16, WIDTH), F32),
            vmem((TILES, BLOCKS, 64, WIDTH), F32),
            vmem((EXT, 64, WIDTH), F32),
            vmem((3, 2, 64, WIDTH), F32),
            vmem((128, LOCAL), BF16),
            pltpu.SMEM((TILES, BLOCKS), jnp.int32),
            pltpu.SMEM((TILES, BLOCKS), jnp.int32),
            pltpu.SMEM((2,), jnp.int32),
            pltpu.SemaphoreType.DMA((2, TILES)),
            pltpu.SemaphoreType.DMA((3,)),
            pltpu.SemaphoreType.DMA((TILES,)),
            pltpu.SemaphoreType.DMA((6,)),
            pltpu.SemaphoreType.DMA((6,)),
            pltpu.SemaphoreType.DMA((10,)),
            pltpu.SemaphoreType.DMA((10,)),
        ],
        compiler_params=pltpu.CompilerParams(
            collective_id=0, has_side_effects=True, vmem_limit_bytes=60 * 1024 * 1024
        ),
    )(basis, k_tiles, m_tiles, tile_part, tile_slot, iface_rows)
    return corrections, theta.reshape(PAIRS)


def solution(mesh):
    in_specs = (
        P(None, AXIS),
        P(AXIS, None, None, None),
        P(AXIS, None, None, None),
        P(AXIS, None),
        P(AXIS, None),
        P(AXIS),
    )
    return jax.shard_map(
        shards, mesh=mesh, in_specs=in_specs, out_specs=(P(None, AXIS), P()), check_vma=False
    )
```

```python
import functools

import jax
import jax.numpy as jnp
from jax import lax
from jax.experimental import pallas as pl
from jax.experimental.pallas import tpu as pltpu
from jax.sharding import PartitionSpec as P

AXIS = "parts"
PARTS = 256
GROUP = 16
FAR = 128
PAIRS = 16
TILES = 8
BLOCKS = 5
WIDTH = 128
LOCAL = TILES * WIDTH
EXT = TILES + 6
RELAX = 0.4
MESH = pl.DeviceIdType.MESH
F32 = jnp.float32
BF16 = jnp.bfloat16
NT = (((1,), (1,)), ((), ()))
TN = (((0,), (0,)), ((), ()))


def split(x):
    hi = x.astype(BF16)
    return hi, (x - hi.astype(F32)).astype(BF16)


def mm(a, b):
    return jnp.dot(a, b, preferred_element_type=F32)


def mm_nt(a, b):
    return lax.dot_general(a, b, NT, preferred_element_type=F32)


def small(a, b, dims=(((1,), (0,)), ((), ()))):
    return lax.dot_general(
        a, b, dims, precision=lax.Precision.HIGHEST, preferred_element_type=F32
    )


def pack4(v):
    return jnp.concatenate([v[4 * i : 4 * i + 4] for i in range(4)], axis=1)


def unpack4(v):
    return jnp.concatenate([v[:, 32 * i : 32 * i + 32] for i in range(4)], axis=0)


def pack2(v):
    flat = jnp.concatenate([v[2 * i : 2 * i + 2] for i in range(8)], axis=1)
    return jnp.stack([flat[:, WIDTH * u : WIDTH * u + WIDTH] for u in range(v.shape[1] // 16)])


def unpack2(v):
    flat = jnp.concatenate([v[u] for u in range(v.shape[0])], axis=1)
    wide = 16 * v.shape[0]
    return jnp.concatenate([flat[:, wide * i : wide * i + wide] for i in range(8)], axis=0)


def eliminate(gram, rows, eye):
    aug = jnp.concatenate([gram, eye], axis=1)
    for j in range(PAIRS):
        pivot = aug[j : j + 1, j : j + 1]
        d = lax.rsqrt(pivot)
        d = d * (1.5 - 0.5 * pivot * d * d)
        line = aug[j : j + 1, :] * d
        col = aug[:, j : j + 1] * d
        aug = jnp.where(rows == j, line, jnp.where(rows > j, aug - col * line, aug))
    return aug[:, PAIRS:]


def kernel(
    scale,
    basis_ref,
    k_ref,
    m_ref,
    part_hbm,
    slot_hbm,
    iface_hbm,
    out_ref,
    theta_ref,
    kbuf,
    mbuf,
    w_hi,
    w_lo,
    xt,
    dinv,
    ext16,
    ext32,
    words,
    s_hi,
    s_lo,
    pt,
    ad,
    right,
    left,
    h0out,
    h1out,
    h2out,
    h3out,
    h0in,
    h1in,
    h2in,
    h3in,
    ar_first,
    ar_big,
    ar_small,
    ar_third,
    ar_extra,
    back,
    adj,
    zin,
    right2,
    part_ref,
    slot_ref,
    iface_ref,
    load_sem,
    index_sem,
    x_sem,
    hs_sem,
    hr_sem,
    as_sem,
    ar_sem,
):
    me = lax.axis_index(AXIS)
    rank_a = lax.rem(me, GROUP)
    base_a = me - rank_a
    rank_b = me // GROUP
    halo_to = (
        lax.rem(me + PARTS - 1, PARTS),
        lax.rem(me + 1, PARTS),
        lax.rem(me + FAR, PARTS),
    )

    def peer_a(k):
        return base_a + lax.rem(rank_a + k, GROUP)

    def peer_b(k):
        return rank_a + GROUP * lax.rem(rank_b + k, GROUP)

    barrier = pltpu.get_barrier_semaphore()

    def greet(k, carry):
        pl.semaphore_signal(barrier, inc=1, device_id=(peer_a(k),), device_id_type=MESH)
        pl.semaphore_signal(barrier, inc=1, device_id=(peer_b(k),), device_id_type=MESH)
        return carry

    lax.fori_loop(1, GROUP, greet, 0, unroll=True)
    for device in halo_to:
        pl.semaphore_signal(barrier, inc=1, device_id=(device,), device_id_type=MESH)

    loads = []
    tables = ((part_hbm, part_ref), (slot_hbm, slot_ref), (iface_hbm, iface_ref))
    for n, (src, dst) in enumerate(tables):
        loads.append(pltpu.make_async_copy(src, dst, index_sem.at[n]))
        loads[-1].start()
    for i in range(TILES):
        loads.append(
            pltpu.make_async_copy(
                basis_ref.at[:, pl.ds(i * WIDTH, WIDTH)], xt.at[i], x_sem.at[i]
            )
        )
        loads[-1].start()
    for i in range(TILES):
        for n, (src, dst) in enumerate(((k_ref, kbuf), (m_ref, mbuf))):
            pltpu.make_async_copy(src.at[i], dst.at[i], load_sem.at[n, i]).start()

    def halo(step, out, into):
        for g, device in enumerate(halo_to):
            pltpu.make_async_remote_copy(
                src_ref=out,
                dst_ref=into.at[g],
                send_sem=hs_sem.at[step],
                recv_sem=hr_sem.at[step],
                device_id=(device,),
                device_id_type=MESH,
            ).start()

    def halo_wait(step, into):
        pltpu.make_async_copy(into, into, hr_sem.at[step]).wait()

    def spread(buf, stage, step, value):
        rank = rank_a if stage == 0 else rank_b
        peer = peer_a if stage == 0 else peer_b
        buf[rank] = value

        def send(k, carry):
            pltpu.make_async_remote_copy(
                src_ref=buf.at[rank],
                dst_ref=buf.at[rank],
                send_sem=as_sem.at[2 * step + stage],
                recv_sem=ar_sem.at[2 * step + stage],
                device_id=(peer(k),),
                device_id_type=MESH,
            ).start()
            return carry

        lax.fori_loop(1, GROUP, send, 0, unroll=True)

    def gathered(buf, stage, step):
        most = buf.at[pl.ds(0, GROUP - 1)]
        pltpu.make_async_copy(most, most, ar_sem.at[2 * step + stage]).wait()
        total = buf[0]
        for j in range(1, GROUP):
            total = total + buf[j]
        return total

    def span(i):
        return pl.ds(i * WIDTH, WIDTH)

    for copy in loads:
        copy.wait()
    columns = []
    for i in range(TILES):
        line = []
        for b in range(BLOCKS):
            part = part_ref[i, b]
            slot = slot_ref[i, b]
            where = jnp.where(
                part == halo_to[1],
                TILES,
                jnp.where(part == halo_to[0], TILES + 2, TILES + 4),
            )
            line.append(jnp.where(part == me, slot, where + slot))
        columns.append(line)
    iface = [iface_ref[0], iface_ref[1]]
    for s in range(2):
        h0out[s] = xt[iface[s]]
    pl.semaphore_wait(barrier, 33)
    halo(0, h0out, h0in)

    eye_w = lax.broadcasted_iota(jnp.int32, (WIDTH, WIDTH), 0) == lax.broadcasted_iota(
        jnp.int32, (WIDTH, WIDTH), 1
    )
    for i in range(TILES):
        hi, lo = split(xt[i])
        ext16[i, 0:16] = hi
        ext16[i, 16:32] = lo
        right[64:80, span(i)] = hi
        right[80:96, span(i)] = lo
        left[0:16, span(i)] = hi
        left[48:64, span(i)] = lo

    def prepare(i, carry):
        for n, (src, dst) in enumerate(((k_ref, kbuf), (m_ref, mbuf))):
            pltpu.make_async_copy(src.at[i], dst.at[i], load_sem.at[n, i]).wait()
            for b in range(BLOCKS):
                hi, lo = split(dst[i, b].T)
                w_hi[i, b * WIDTH : (b + 1) * WIDTH, n * WIDTH : (n + 1) * WIDTH] = hi
                w_lo[i, b * WIDTH : (b + 1) * WIDTH, n * WIDTH : (n + 1) * WIDTH] = lo
        diagonal = jnp.sum(jnp.where(eye_w, kbuf[i, 0], 0.0), axis=0, keepdims=True)
        dinv[i] = jnp.broadcast_to(1.0 / diagonal, (8, WIDTH))
        return carry

    lax.fori_loop(0, TILES, prepare, 0)
    d = [dinv[i, 0:1] for i in range(TILES)]
    for i in range(TILES):
        hi, lo = split(xt[i] * d[i])
        right[16:32, span(i)] = hi
        right[48:64, span(i)] = lo

    def apply(ext, rows, i):
        picked = jnp.concatenate([ext[columns[i][b]] for b in range(BLOCKS)], axis=1)
        high = mm(picked, w_hi[i])
        low = mm(picked[:rows], w_lo[i])
        return high[:rows] + high[rows:] + low

    halo_wait(0, h0in)
    for g in range(3):
        for s in range(2):
            hi, lo = split(h0in[g, s])
            ext16[TILES + 2 * g + s, 0:16] = hi
            ext16[TILES + 2 * g + s, 16:32] = lo
    for i in range(TILES):
        y = apply(ext16, 16, i)
        p, q = y[:, :WIDTH], y[:, WIDTH:]
        words[i, 0:16] = p * d[i]
        words[i, 16:32] = q * d[i]
        hi, lo = split(p)
        left[16:32, span(i)] = hi
        left[64:80, span(i)] = lo
        hi, lo = split(q)
        left[32:48, span(i)] = hi
        left[80:96, span(i)] = lo
        right[0:16, span(i)] = hi
        right[32:48, span(i)] = lo
    for s in range(2):
        h1out[s] = words[iface[s], 0:32]
    halo(1, h1out, h1in)

    gram = mm_nt(left[0:96], right[...])
    gram = gram[0:48] + gram[48:96]
    with_qx = gram[:, 0:32] + gram[:, 32:64]
    with_x = gram[:, 64:80] + gram[:, 80:96]
    payload = pack2(
        jnp.concatenate([with_qx[16:32], with_qx[32:48], with_x[0:16]], axis=1)
    )
    spread(ar_first.at[0], 0, 0, payload)

    for i in range(TILES):
        hi, lo = split(words[i, 0:32])
        ext32[i, 0:32] = hi
        ext32[i, 32:64] = lo
        s_hi[i, 0:32] = hi
        s_lo[i, 0:32] = lo
    for i in range(TILES):
        hi, lo = right[0:32, span(i)], right[32:64, span(i)]
        none = jnp.zeros((32, WIDTH), BF16)
        hi = jnp.concatenate(
            [jnp.concatenate([hi, none], axis=1), jnp.concatenate([none, hi], axis=1)], axis=0
        )
        lo = jnp.concatenate(
            [jnp.concatenate([lo, none], axis=1), jnp.concatenate([none, lo], axis=1)], axis=0
        )
        high = mm_nt(jnp.concatenate([hi, lo], axis=0), w_hi[i])
        share = high[0:64] + high[64:128] + mm_nt(hi, w_lo[i])
        for b in range(BLOCKS):
            back[i, b] = share[:, b * WIDTH : (b + 1) * WIDTH]

    def collect(j, total):
        for i in range(TILES):
            for b in range(1, BLOCKS):
                total = total + jnp.where(columns[i][b] == j, back[i, b], 0.0)
        adj[j] = total

    def collect_remote(j, carry):
        collect(j, jnp.zeros((64, WIDTH), F32))
        return carry

    def collect_local(j, carry):
        collect(j, back[j, 0])
        return carry

    lax.fori_loop(TILES, EXT, collect_remote, 0)
    for g, device in enumerate((halo_to[1], halo_to[0], halo_to[2])):
        pltpu.make_async_remote_copy(
            src_ref=adj.at[pl.ds(TILES + 2 * g, 2)],
            dst_ref=zin.at[g],
            send_sem=hs_sem.at[5],
            recv_sem=hr_sem.at[5],
            device_id=(device,),
            device_id_type=MESH,
        ).start()
    halo_wait(1, h1in)
    for g in range(3):
        for s in range(2):
            hi, lo = split(h1in[g, s])
            t = TILES + 2 * g + s
            ext32[t, 0:32] = hi
            ext32[t, 32:64] = lo
            s_hi[t, 0:32] = hi
            s_lo[t, 0:32] = lo

    for i in range(TILES):
        if i == 0:
            spread(ar_first.at[1], 1, 0, gathered(ar_first.at[0], 0, 0))
        y = apply(ext32, 32, i)
        stiff, mass = y[:, :WIDTH], y[:, WIDTH:]
        hi, lo = split(stiff)
        left[0:32, span(i)] = hi
        left[64:96, span(i)] = lo
        hi, lo = split(mass)
        left[32:64, span(i)] = hi
        left[96:128, span(i)] = lo
        stiff, mass = stiff * d[i], mass * d[i]
        words[i, 32:48] = stiff[16:32]
        words[i, 48:64] = mass[16:32]
        words[i, 64:80] = stiff[0:16]
        words[i, 80:96] = mass[0:16]
    for s in range(2):
        h2out[s] = words[iface[s], 32:96]
    halo(2, h2out, h2in)
    gram = mm_nt(left[...], right[0:64])
    gram = gram[0:64] + gram[64:128]
    gram = gram[:, 0:32] + gram[:, 32:64]
    kept = gram[16:32]
    payload = pack2(jnp.concatenate([gram[0:16], kept + gram[32:48], gram[48:64]], axis=1))
    spread(ar_big.at[0], 0, 1, payload)
    for i in range(TILES):
        hi, lo = split(words[i, 32:96])
        s_hi[i, 32:96] = hi
        s_lo[i, 32:96] = lo
    lax.fori_loop(0, TILES, collect_local, 0)

    def with_back(both, rows):
        gram = mm_nt(both, right2[...])
        gram = gram[0:rows] + gram[rows : 2 * rows]
        return gram[:, 0:64] + gram[:, 64:128]

    pltpu.make_async_copy(zin, zin, hr_sem.at[5]).wait()
    for j in range(TILES):
        total = adj[j]
        for s in range(2):
            for g in range(3):
                total = total + jnp.where(iface[s] == j, zin[g, s], 0.0)
        hi, lo = split(total)
        right2[0:64, span(j)] = hi
        right2[64:128, span(j)] = lo
    both = jnp.concatenate(
        [
            jnp.concatenate([s_hi[t, 32:64] for t in range(TILES)], axis=1),
            jnp.concatenate([s_lo[t, 32:64] for t in range(TILES)], axis=1),
        ],
        axis=0,
    )
    gram = with_back(both, 32)
    middle = gram[0:16, 32:64] + gram[16:32, 0:32]
    spread(
        ar_extra.at[0],
        0,
        4,
        pack2(jnp.concatenate([gram[0:16, 0:32], middle, gram[16:32, 32:64], kept], axis=1)),
    )


    total = gathered(ar_first.at[1], 1, 0) * scale
    total = unpack2(total)
    g_p, g_q, g_xx = total[:, 0:32], total[:, 32:64], total[:, 64:80]
    g_pq, g_px = g_p[:, 0:16], g_p[:, 16:32]
    g_qq, g_qx = g_q[:, 0:16], g_q[:, 16:32]
    row_no = lax.broadcasted_iota(jnp.int32, (PAIRS, 2 * PAIRS), 0)
    eye_b = lax.broadcasted_iota(jnp.int32, (PAIRS, PAIRS), 0) == lax.broadcasted_iota(
        jnp.int32, (PAIRS, PAIRS), 1
    )
    eye = jnp.where(eye_b, 1.0, 0.0).astype(F32)
    inv_v = eliminate(g_xx, row_no, eye)
    inv_m = eliminate(g_qq, row_no, eye)
    projected = small(inv_m, g_pq, NT)
    diag_v = jnp.sum(jnp.where(eye_b, inv_v, 0.0), axis=1, keepdims=True)
    diag_m = jnp.sum(jnp.where(eye_b, inv_m, 0.0), axis=1, keepdims=True)
    theta = jnp.sum(projected * inv_v, axis=1, keepdims=True) * diag_m / diag_v
    theta_ref[...] = jnp.sum(jnp.where(eye_b, theta, 0.0), axis=0, keepdims=True)
    wide = jnp.broadcast_to(theta, (PAIRS, WIDTH))
    gram_v = small(inv_v, inv_v, TN)
    gram_m = small(inv_m, inv_m, TN)
    start_p = -RELAX * inv_v
    start_q = RELAX * theta * inv_v
    start_x = small(start_p, g_px) + small(start_q, g_qx)
    r = small(start_x, gram_v)
    pq_m = small(g_pq, gram_m)
    qx_v = small(g_qx, gram_v)
    r_m = small(r, pq_m)
    coef = jnp.concatenate(
        [
            2.0 * start_p + RELAX * r,
            2.0 * start_q,
            -RELAX * start_q,
            RELAX * theta * start_q,
            -RELAX * start_p,
            RELAX * theta * start_p,
        ],
        axis=1,
    )
    halo_wait(2, h2in)
    for g in range(3):
        for s in range(2):
            hi, lo = split(h2in[g, s])
            t = TILES + 2 * g + s
            s_hi[t, 32:96] = hi
            s_lo[t, 32:96] = lo

    def combine(coef, rows, t):
        hi, lo = split(coef)
        both = jnp.concatenate([hi, lo], axis=0)
        first = mm(both, s_hi[t, 0:rows])
        second = mm(hi, s_lo[t, 0:rows])
        return first[0:16] + first[16:32] + second

    for t in range(EXT):
        p = combine(coef, 96, t)
        pt[t] = p
        hi, lo = split(p)
        ext16[t, 0:16] = hi
        ext16[t, 16:32] = lo

    def residual(step):
        for i in range(TILES):
            if i == 4 and step == 1:
                spread(ar_big.at[1], 1, 1, gathered(ar_big.at[0], 0, 1))
            if i == 4 and step == 2:
                spread(ar_small.at[1], 1, 2, gathered(ar_small.at[0], 0, 2))
            y = apply(ext16, 16, i)
            image = y[:, :WIDTH] - wide * y[:, WIDTH:]
            moved = image * d[i]
            ad[i] = moved
            if step < 3:
                hi, lo = split(image)
                left[0:16, span(i)] = hi
                left[16:32, span(i)] = lo
            if step == 2:
                hi, lo = split(moved)
                left[32:48, span(i)] = hi
                left[48:64, span(i)] = lo
        if step < 3:
            out = h3out.at[step - 1]
            for s in range(2):
                out[s] = ad[iface[s]]
            halo(step + 2, out, h3in.at[step - 1])

    def with_qxd(rows):
        gram = mm_nt(left[0 : 2 * rows], right[0:64])
        gram = gram[0:rows] + gram[rows : 2 * rows]
        return gram[:, 0:32] + gram[:, 32:64]

    residual(1)
    gram = with_qxd(16)
    spread(ar_small.at[0], 0, 2, pack4(gram))

    spread(ar_extra.at[1], 1, 4, gathered(ar_extra.at[0], 0, 4))
    total = unpack2(gathered(ar_big.at[1], 1, 1)) * scale
    kp, kq_mp, mq = total[:, 0:32], total[:, 32:64], total[:, 64:96]
    image = -RELAX * (
        small(inv_v, kp) - theta * (small(inv_v, kq_mp) - theta * small(inv_v, mq))
    )
    p_x = 2.0 * start_x - RELAX * image[:, 16:32] + RELAX * small(r, g_px)

    def advance(image, r_m, p_x):
        m = small(image[:, 0:16], gram_m) - r_m
        r = small(p_x, gram_v) + RELAX * small(m, qx_v)
        return m, p_x + RELAX * small(m, g_qx), r

    def coefficients(m, r):
        parts = [
            start_p + RELAX * r,
            start_q + RELAX * m,
            -RELAX * RELAX * m,
            RELAX * RELAX * theta * m,
        ]
        return jnp.concatenate(parts, axis=1)

    def image_of(m):
        return RELAX * (small(m, kq) - theta * small(m, mq))

    for step in (1, 2):
        m, c_x, r = advance(image, r_m, p_x)
        coef = coefficients(m, r)
        for t in range(TILES):
            p = pt[t] - RELAX * ad[t] + combine(coef, 64, t)
            pt[t] = p
            hi, lo = split(p)
            ext16[t, 0:16] = hi
            ext16[t, 16:32] = lo
        for t in range(TILES, EXT):
            pt[t] = pt[t] + combine(coef, 64, t)
        if step == 2:
            spread(ar_third.at[1], 1, 3, gathered(ar_third.at[0], 0, 3))
        halo_wait(step + 2, h3in.at[step - 1])
        for g in range(3):
            for s in range(2):
                t = TILES + 2 * g + s
                p = pt[t] - RELAX * h3in[step - 1, g, s]
                pt[t] = p
                hi, lo = split(p)
                ext16[t, 0:16] = hi
                ext16[t, 16:32] = lo
        residual(step + 1)
        r_px = small(r, g_px)
        r_m = small(r, pq_m)
        if step == 1:
            gram = with_qxd(16)
            gram_b = with_back(left[32:64], 16)
            gram_b = gram_b[:, 0:32] - theta * gram_b[:, 32:64]
            spread(ar_third.at[0], 0, 3, jnp.stack([pack4(gram), pack4(gram_b)]))
            extra = unpack2(gathered(ar_extra.at[1], 1, 4)) * scale
            kq = extra[:, 96:128]
            mp = kq_mp - kq
            m_image = image_of(m)
            image = unpack4(gathered(ar_small.at[1], 1, 2)) * scale + m_image
            p_x = c_x + start_x - RELAX * image[:, 16:32] + RELAX * r_px

    m_image = image_of(m)
    near = coef[:, 0:32]
    twice = small(m, extra[:, 0:32]) - theta * (
        small(m, extra[:, 32:64]) - theta * small(m, extra[:, 64:96])
    )
    known = small(near, jnp.concatenate([kp, kq], axis=0)) - theta * small(
        near, jnp.concatenate([mp, mq], axis=0)
    )
    known = known - RELAX * RELAX * twice
    total = gathered(ar_third.at[1], 1, 3) * scale
    image = unpack4(total[0])
    known = known + image - RELAX * unpack4(total[1])
    image = image + m_image
    p_x = c_x + start_x - RELAX * image[:, 16:32] + RELAX * r_px
    m, c_x, r = advance(image, r_m, p_x)
    coef = coefficients(m, r)
    image = known + image_of(m)
    r_m = small(r, pq_m)
    p_x = c_x + start_x - RELAX * image[:, 16:32] + RELAX * small(r, g_px)
    for t in range(TILES):
        pt[t] = pt[t] - RELAX * ad[t] + combine(coef, 64, t)

    m, c_x, r = advance(image, r_m, p_x)
    q_hi, q_lo = split(RELAX * m)
    x_hi, x_lo = split(-r)
    lead = jnp.concatenate([q_hi, x_hi], axis=1)
    rest = jnp.concatenate([q_lo, x_lo], axis=1)
    for t in range(TILES):
        hi = jnp.concatenate([s_hi[t, 16:32], right[64:80, span(t)]], axis=0)
        lo = jnp.concatenate([s_lo[t, 16:32], right[80:96, span(t)]], axis=0)
        out_ref[:, span(t)] = pt[t] + (mm(lead, hi) + mm(rest, hi) + mm(lead, lo))

    for step, out in enumerate((h0out, h1out, h2out, h3out.at[0], h3out.at[1])):
        for g in range(3):
            pltpu.make_async_copy(out, out, hs_sem.at[step]).wait()
    sent = adj.at[pl.ds(TILES, 6)]
    pltpu.make_async_copy(sent, sent, hs_sem.at[5]).wait()
    for step, buf in enumerate((ar_first, ar_big, ar_small, ar_third, ar_extra)):
        for stage in range(2):
            most = buf.at[stage, pl.ds(0, GROUP - 1)]
            pltpu.make_async_copy(most, most, as_sem.at[2 * step + stage]).wait()


def shards(basis, k_tiles, m_tiles, tile_part, tile_slot, iface_rows):
    rows = basis.shape[1] * lax.axis_size(AXIS)
    vmem = pltpu.VMEM
    corrections, theta = pl.pallas_call(
        functools.partial(kernel, 1.0 / rows),
        out_shape=(
            pltpu.VMEM((PAIRS, LOCAL), F32),
            pltpu.VMEM((1, PAIRS), F32),
        ),
        in_specs=[pl.BlockSpec(memory_space=pltpu.HBM)] * 6,
        out_specs=(pl.BlockSpec(memory_space=vmem), pl.BlockSpec(memory_space=vmem)),
        scratch_shapes=[
            vmem((TILES, BLOCKS, WIDTH, WIDTH), F32),
            vmem((TILES, BLOCKS, WIDTH, WIDTH), F32),
            vmem((TILES, BLOCKS * WIDTH, 2 * WIDTH), BF16),
            vmem((TILES, BLOCKS * WIDTH, 2 * WIDTH), BF16),
            vmem((TILES, 16, WIDTH), F32),
            vmem((TILES, 8, WIDTH), F32),
            vmem((EXT, 32, WIDTH), BF16),
            vmem((EXT, 64, WIDTH), BF16),
            vmem((TILES, 96, WIDTH), F32),
            vmem((EXT, 96, WIDTH), BF16),
            vmem((EXT, 96, WIDTH), BF16),
            vmem((EXT, 16, WIDTH), F32),
            vmem((TILES, 16, WIDTH), F32),
            vmem((96, LOCAL), BF16),
            vmem((128, LOCAL), BF16),
            vmem((2, 16, WIDTH), F32),
            vmem((2, 32, WIDTH), F32),
            vmem((2, 64, WIDTH), F32),
            vmem((2, 2, 16, WIDTH), F32),
            vmem((3, 2, 16, WIDTH), F32),
            vmem((3, 2, 32, WIDTH), F32),
            vmem((3, 2, 64, WIDTH), F32),
            vmem((2, 3, 2, 16, WIDTH), F32),
            vmem((2, GROUP, 5, 2, WIDTH), F32),
            vmem((2, GROUP, 6, 2, WIDTH), F32),
            vmem((2, GROUP, 4, WIDTH), F32),
            vmem((2, GROUP, 2, 4, WIDTH), F32),
            vmem((2, GROUP, 8, 2, WIDTH), F32),
            vmem((TILES, BLOCKS, 64, WIDTH), F32),
            vmem((EXT, 64, WIDTH), F32),
            vmem((3, 2, 64, WIDTH), F32),
            vmem((128, LOCAL), BF16),
            pltpu.SMEM((TILES, BLOCKS), jnp.int32),
            pltpu.SMEM((TILES, BLOCKS), jnp.int32),
            pltpu.SMEM((2,), jnp.int32),
            pltpu.SemaphoreType.DMA((2, TILES)),
            pltpu.SemaphoreType.DMA((3,)),
            pltpu.SemaphoreType.DMA((TILES,)),
            pltpu.SemaphoreType.DMA((6,)),
            pltpu.SemaphoreType.DMA((6,)),
            pltpu.SemaphoreType.DMA((10,)),
            pltpu.SemaphoreType.DMA((10,)),
        ],
        compiler_params=pltpu.CompilerParams(
            collective_id=0, has_side_effects=True, vmem_limit_bytes=60 * 1024 * 1024
        ),
    )(basis, k_tiles, m_tiles, tile_part, tile_slot, iface_rows)
    return corrections, theta.reshape(PAIRS)


def solution(mesh):
    in_specs = (
        P(None, AXIS),
        P(AXIS, None, None, None),
        P(AXIS, None, None, None),
        P(AXIS, None),
        P(AXIS, None),
        P(AXIS),
    )
    return jax.shard_map(
        shards, mesh=mesh, in_specs=in_specs, out_specs=(P(None, AXIS), P()), check_vma=False
    )
```

```python
import functools

import jax
import jax.numpy as jnp
from jax import lax
from jax.experimental import pallas as pl
from jax.experimental.pallas import tpu as pltpu
from jax.sharding import PartitionSpec as P

AXIS = "parts"
PARTS = 256
GROUP = 16
FAR = 128
PAIRS = 16
TILES = 8
BLOCKS = 5
WIDTH = 128
LOCAL = TILES * WIDTH
EXT = TILES + 6
RELAX = 0.4
MESH = pl.DeviceIdType.MESH
ORDER_A = (8, 7, 9, 6, 10, 5, 11, 4, 12, 3, 13, 2, 14, 1, 15)
ORDER_B = (10, 6, 14, 9, 11, 2, 8, 5, 7, 13, 15, 1, 3, 4, 12)
F32 = jnp.float32
BF16 = jnp.bfloat16
NT = (((1,), (1,)), ((), ()))
TN = (((0,), (0,)), ((), ()))


def split(x):
    hi = x.astype(BF16)
    return hi, (x - hi.astype(F32)).astype(BF16)


def mm(a, b):
    return jnp.dot(a, b, preferred_element_type=F32)


def mm_nt(a, b):
    return lax.dot_general(a, b, NT, preferred_element_type=F32)


def small(a, b, dims=(((1,), (0,)), ((), ()))):
    return lax.dot_general(
        a, b, dims, precision=lax.Precision.HIGHEST, preferred_element_type=F32
    )


def pack4(v):
    return jnp.concatenate([v[4 * i : 4 * i + 4] for i in range(4)], axis=1)


def unpack4(v):
    return jnp.concatenate([v[:, 32 * i : 32 * i + 32] for i in range(4)], axis=0)


def pack2(v):
    flat = jnp.concatenate([v[2 * i : 2 * i + 2] for i in range(8)], axis=1)
    return jnp.stack([flat[:, WIDTH * u : WIDTH * u + WIDTH] for u in range(v.shape[1] // 16)])


def unpack2(v):
    flat = jnp.concatenate([v[u] for u in range(v.shape[0])], axis=1)
    wide = 16 * v.shape[0]
    return jnp.concatenate([flat[:, wide * i : wide * i + wide] for i in range(8)], axis=0)


def eliminate(gram, rows, eye):
    aug = jnp.concatenate([gram, eye], axis=1)
    for j in range(PAIRS):
        pivot = aug[j : j + 1, j : j + 1]
        d = lax.rsqrt(pivot)
        d = d * (1.5 - 0.5 * pivot * d * d)
        line = aug[j : j + 1, :] * d
        col = aug[:, j : j + 1] * d
        aug = jnp.where(rows == j, line, jnp.where(rows > j, aug - col * line, aug))
    return aug[:, PAIRS:]


def kernel(
    scale,
    basis_ref,
    k_ref,
    m_ref,
    part_hbm,
    slot_hbm,
    iface_hbm,
    out_ref,
    theta_ref,
    kbuf,
    mbuf,
    w_hi,
    w_lo,
    xt,
    dinv,
    ext16,
    ext32,
    words,
    s_hi,
    s_lo,
    pt,
    ad,
    right,
    left,
    h0out,
    h1out,
    h2out,
    h3out,
    h0in,
    h1in,
    h2in,
    h3in,
    ar_first,
    ar_big,
    ar_small,
    ar_third,
    ar_extra,
    back,
    adj,
    zin,
    right2,
    part_ref,
    slot_ref,
    iface_ref,
    load_sem,
    index_sem,
    x_sem,
    hs_sem,
    hr_sem,
    as_sem,
    ar_sem,
):
    me = lax.axis_index(AXIS)
    rank_a = lax.rem(me, GROUP)
    base_a = me - rank_a
    rank_b = me // GROUP
    halo_to = (
        lax.rem(me + PARTS - 1, PARTS),
        lax.rem(me + 1, PARTS),
        lax.rem(me + FAR, PARTS),
    )

    def peer_a(k):
        return base_a + lax.rem(rank_a + k, GROUP)

    def peer_b(k):
        across = lax.rem(lax.rem(rank_b, 4) + k % 4, 4)
        along = lax.rem(rank_b // 4 + k // 4, 4)
        return rank_a + GROUP * (4 * along + across)

    barrier = pltpu.get_barrier_semaphore()

    for near, far in zip(ORDER_A, ORDER_B):
        for device in (peer_b(far), peer_a(near)):
            pl.semaphore_signal(barrier, inc=1, device_id=(device,), device_id_type=MESH)
    for device in halo_to:
        pl.semaphore_signal(barrier, inc=1, device_id=(device,), device_id_type=MESH)

    loads = []
    tables = ((part_hbm, part_ref), (slot_hbm, slot_ref), (iface_hbm, iface_ref))
    for n, (src, dst) in enumerate(tables):
        loads.append(pltpu.make_async_copy(src, dst, index_sem.at[n]))
        loads[-1].start()
    for i in range(TILES):
        loads.append(
            pltpu.make_async_copy(
                basis_ref.at[:, pl.ds(i * WIDTH, WIDTH)], xt.at[i], x_sem.at[i]
            )
        )
        loads[-1].start()
    for i in range(TILES):
        for n, (src, dst) in enumerate(((k_ref, kbuf), (m_ref, mbuf))):
            pltpu.make_async_copy(src.at[i], dst.at[i], load_sem.at[n, i]).start()

    def halo(step, out, into):
        for g, device in enumerate(halo_to):
            pltpu.make_async_remote_copy(
                src_ref=out,
                dst_ref=into.at[g],
                send_sem=hs_sem.at[step],
                recv_sem=hr_sem.at[step],
                device_id=(device,),
                device_id_type=MESH,
            ).start()

    def halo_wait(step, into):
        pltpu.make_async_copy(into, into, hr_sem.at[step]).wait()

    def spread(buf, stage, step, value):
        rank = rank_a if stage == 0 else rank_b
        peer = peer_a if stage == 0 else peer_b
        buf[rank] = value

        for k in ORDER_A if stage == 0 else ORDER_B:
            pltpu.make_async_remote_copy(
                src_ref=buf.at[rank],
                dst_ref=buf.at[rank],
                send_sem=as_sem.at[2 * step + stage],
                recv_sem=ar_sem.at[2 * step + stage],
                device_id=(peer(k),),
                device_id_type=MESH,
            ).start()

    def gathered(buf, stage, step):
        most = buf.at[pl.ds(0, GROUP - 1)]
        pltpu.make_async_copy(most, most, ar_sem.at[2 * step + stage]).wait()
        total = buf[0]
        for j in range(1, GROUP):
            total = total + buf[j]
        return total

    def span(i):
        return pl.ds(i * WIDTH, WIDTH)

    for copy in loads:
        copy.wait()
    columns = []
    for i in range(TILES):
        line = []
        for b in range(BLOCKS):
            part = part_ref[i, b]
            slot = slot_ref[i, b]
            where = jnp.where(
                part == halo_to[1],
                TILES,
                jnp.where(part == halo_to[0], TILES + 2, TILES + 4),
            )
            line.append(jnp.where(part == me, slot, where + slot))
        columns.append(line)
    iface = [iface_ref[0], iface_ref[1]]
    for s in range(2):
        h0out[s] = xt[iface[s]]
    pl.semaphore_wait(barrier, 33)
    halo(0, h0out, h0in)

    eye_w = lax.broadcasted_iota(jnp.int32, (WIDTH, WIDTH), 0) == lax.broadcasted_iota(
        jnp.int32, (WIDTH, WIDTH), 1
    )
    for i in range(TILES):
        hi, lo = split(xt[i])
        ext16[i, 0:16] = hi
        ext16[i, 16:32] = lo
        right[64:80, span(i)] = hi
        right[80:96, span(i)] = lo
        left[0:16, span(i)] = hi
        left[48:64, span(i)] = lo

    def prepare(i, carry):
        for n, (src, dst) in enumerate(((k_ref, kbuf), (m_ref, mbuf))):
            pltpu.make_async_copy(src.at[i], dst.at[i], load_sem.at[n, i]).wait()
            for b in range(BLOCKS):
                hi, lo = split(dst[i, b].T)
                w_hi[i, b * WIDTH : (b + 1) * WIDTH, n * WIDTH : (n + 1) * WIDTH] = hi
                w_lo[i, b * WIDTH : (b + 1) * WIDTH, n * WIDTH : (n + 1) * WIDTH] = lo
        diagonal = jnp.sum(jnp.where(eye_w, kbuf[i, 0], 0.0), axis=0, keepdims=True)
        dinv[i] = jnp.broadcast_to(1.0 / diagonal, (8, WIDTH))
        return carry

    lax.fori_loop(0, TILES, prepare, 0)
    d = [dinv[i, 0:1] for i in range(TILES)]
    for i in range(TILES):
        hi, lo = split(xt[i] * d[i])
        right[16:32, span(i)] = hi
        right[48:64, span(i)] = lo

    def apply(ext, rows, i):
        picked = jnp.concatenate([ext[columns[i][b]] for b in range(BLOCKS)], axis=1)
        high = mm(picked, w_hi[i])
        low = mm(picked[:rows], w_lo[i])
        return high[:rows] + high[rows:] + low

    halo_wait(0, h0in)
    for g in range(3):
        for s in range(2):
            hi, lo = split(h0in[g, s])
            ext16[TILES + 2 * g + s, 0:16] = hi
            ext16[TILES + 2 * g + s, 16:32] = lo
    for i in range(TILES):
        y = apply(ext16, 16, i)
        p, q = y[:, :WIDTH], y[:, WIDTH:]
        words[i, 0:16] = p * d[i]
        words[i, 16:32] = q * d[i]
        hi, lo = split(p)
        left[16:32, span(i)] = hi
        left[64:80, span(i)] = lo
        hi, lo = split(q)
        left[32:48, span(i)] = hi
        left[80:96, span(i)] = lo
        right[0:16, span(i)] = hi
        right[32:48, span(i)] = lo
    for s in range(2):
        h1out[s] = words[iface[s], 0:32]
    halo(1, h1out, h1in)

    gram = mm_nt(left[0:96], right[...])
    gram = gram[0:48] + gram[48:96]
    with_qx = gram[:, 0:32] + gram[:, 32:64]
    with_x = gram[:, 64:80] + gram[:, 80:96]
    payload = pack2(
        jnp.concatenate([with_qx[16:32], with_qx[32:48], with_x[0:16]], axis=1)
    )
    spread(ar_first.at[0], 0, 0, payload)

    for i in range(TILES):
        hi, lo = split(words[i, 0:32])
        ext32[i, 0:32] = hi
        ext32[i, 32:64] = lo
        s_hi[i, 0:32] = hi
        s_lo[i, 0:32] = lo
    for i in range(TILES):
        hi, lo = right[0:32, span(i)], right[32:64, span(i)]
        none = jnp.zeros((32, WIDTH), BF16)
        hi = jnp.concatenate(
            [jnp.concatenate([hi, none], axis=1), jnp.concatenate([none, hi], axis=1)], axis=0
        )
        lo = jnp.concatenate(
            [jnp.concatenate([lo, none], axis=1), jnp.concatenate([none, lo], axis=1)], axis=0
        )
        high = mm_nt(jnp.concatenate([hi, lo], axis=0), w_hi[i])
        share = high[0:64] + high[64:128] + mm_nt(hi, w_lo[i])
        for b in range(BLOCKS):
            back[i, b] = share[:, b * WIDTH : (b + 1) * WIDTH]

    def collect(j, total):
        for i in range(TILES):
            for b in range(1, BLOCKS):
                total = total + jnp.where(columns[i][b] == j, back[i, b], 0.0)
        adj[j] = total

    def collect_remote(j, carry):
        collect(j, jnp.zeros((64, WIDTH), F32))
        return carry

    def collect_local(j, carry):
        collect(j, back[j, 0])
        return carry

    lax.fori_loop(TILES, EXT, collect_remote, 0)
    for g, device in enumerate((halo_to[1], halo_to[0], halo_to[2])):
        pltpu.make_async_remote_copy(
            src_ref=adj.at[pl.ds(TILES + 2 * g, 2)],
            dst_ref=zin.at[g],
            send_sem=hs_sem.at[5],
            recv_sem=hr_sem.at[5],
            device_id=(device,),
            device_id_type=MESH,
        ).start()
    halo_wait(1, h1in)
    for g in range(3):
        for s in range(2):
            hi, lo = split(h1in[g, s])
            t = TILES + 2 * g + s
            ext32[t, 0:32] = hi
            ext32[t, 32:64] = lo
            s_hi[t, 0:32] = hi
            s_lo[t, 0:32] = lo

    for i in range(TILES):
        if i == 0:
            spread(ar_first.at[1], 1, 0, gathered(ar_first.at[0], 0, 0))
        y = apply(ext32, 32, i)
        stiff, mass = y[:, :WIDTH], y[:, WIDTH:]
        hi, lo = split(stiff)
        left[0:32, span(i)] = hi
        left[64:96, span(i)] = lo
        hi, lo = split(mass)
        left[32:64, span(i)] = hi
        left[96:128, span(i)] = lo
        stiff, mass = stiff * d[i], mass * d[i]
        words[i, 32:48] = stiff[16:32]
        words[i, 48:64] = mass[16:32]
        words[i, 64:80] = stiff[0:16]
        words[i, 80:96] = mass[0:16]
    for s in range(2):
        h2out[s] = words[iface[s], 32:96]
    halo(2, h2out, h2in)
    gram = mm_nt(left[...], right[0:64])
    gram = gram[0:64] + gram[64:128]
    gram = gram[:, 0:32] + gram[:, 32:64]
    kept = gram[16:32]
    payload = pack2(jnp.concatenate([gram[0:16], kept + gram[32:48], gram[48:64]], axis=1))
    spread(ar_big.at[0], 0, 1, payload)
    for i in range(TILES):
        hi, lo = split(words[i, 32:96])
        s_hi[i, 32:96] = hi
        s_lo[i, 32:96] = lo
    lax.fori_loop(0, TILES, collect_local, 0)

    def with_back(both, rows):
        gram = mm_nt(both, right2[...])
        gram = gram[0:rows] + gram[rows : 2 * rows]
        return gram[:, 0:64] + gram[:, 64:128]

    pltpu.make_async_copy(zin, zin, hr_sem.at[5]).wait()
    for j in range(TILES):
        total = adj[j]
        for s in range(2):
            for g in range(3):
                total = total + jnp.where(iface[s] == j, zin[g, s], 0.0)
        hi, lo = split(total)
        right2[0:64, span(j)] = hi
        right2[64:128, span(j)] = lo
    both = jnp.concatenate(
        [
            jnp.concatenate([s_hi[t, 32:64] for t in range(TILES)], axis=1),
            jnp.concatenate([s_lo[t, 32:64] for t in range(TILES)], axis=1),
        ],
        axis=0,
    )
    gram = with_back(both, 32)
    middle = gram[0:16, 32:64] + gram[16:32, 0:32]
    spread(
        ar_extra.at[0],
        0,
        4,
        pack2(jnp.concatenate([gram[0:16, 0:32], middle, gram[16:32, 32:64], kept], axis=1)),
    )


    total = gathered(ar_first.at[1], 1, 0) * scale
    total = unpack2(total)
    g_p, g_q, g_xx = total[:, 0:32], total[:, 32:64], total[:, 64:80]
    g_pq, g_px = g_p[:, 0:16], g_p[:, 16:32]
    g_qq, g_qx = g_q[:, 0:16], g_q[:, 16:32]
    row_no = lax.broadcasted_iota(jnp.int32, (PAIRS, 2 * PAIRS), 0)
    eye_b = lax.broadcasted_iota(jnp.int32, (PAIRS, PAIRS), 0) == lax.broadcasted_iota(
        jnp.int32, (PAIRS, PAIRS), 1
    )
    eye = jnp.where(eye_b, 1.0, 0.0).astype(F32)
    inv_v = eliminate(g_xx, row_no, eye)
    inv_m = eliminate(g_qq, row_no, eye)
    projected = small(inv_m, g_pq, NT)
    diag_v = jnp.sum(jnp.where(eye_b, inv_v, 0.0), axis=1, keepdims=True)
    diag_m = jnp.sum(jnp.where(eye_b, inv_m, 0.0), axis=1, keepdims=True)
    theta = jnp.sum(projected * inv_v, axis=1, keepdims=True) * diag_m / diag_v
    theta_ref[...] = jnp.sum(jnp.where(eye_b, theta, 0.0), axis=0, keepdims=True)
    wide = jnp.broadcast_to(theta, (PAIRS, WIDTH))
    gram_v = small(inv_v, inv_v, TN)
    gram_m = small(inv_m, inv_m, TN)
    start_p = -RELAX * inv_v
    start_q = RELAX * theta * inv_v
    start_x = small(start_p, g_px) + small(start_q, g_qx)
    r = small(start_x, gram_v)
    pq_m = small(g_pq, gram_m)
    qx_v = small(g_qx, gram_v)
    r_m = small(r, pq_m)
    coef = jnp.concatenate(
        [
            2.0 * start_p + RELAX * r,
            2.0 * start_q,
            -RELAX * start_q,
            RELAX * theta * start_q,
            -RELAX * start_p,
            RELAX * theta * start_p,
        ],
        axis=1,
    )
    halo_wait(2, h2in)
    for g in range(3):
        for s in range(2):
            hi, lo = split(h2in[g, s])
            t = TILES + 2 * g + s
            s_hi[t, 32:96] = hi
            s_lo[t, 32:96] = lo

    def combine(coef, rows, t):
        hi, lo = split(coef)
        both = jnp.concatenate([hi, lo], axis=0)
        first = mm(both, s_hi[t, 0:rows])
        second = mm(hi, s_lo[t, 0:rows])
        return first[0:16] + first[16:32] + second

    for t in range(EXT):
        p = combine(coef, 96, t)
        pt[t] = p
        hi, lo = split(p)
        ext16[t, 0:16] = hi
        ext16[t, 16:32] = lo

    def residual(step):
        for i in range(TILES):
            if i == 4 and step == 1:
                spread(ar_big.at[1], 1, 1, gathered(ar_big.at[0], 0, 1))
            if i == 4 and step == 2:
                spread(ar_small.at[1], 1, 2, gathered(ar_small.at[0], 0, 2))
            y = apply(ext16, 16, i)
            image = y[:, :WIDTH] - wide * y[:, WIDTH:]
            moved = image * d[i]
            ad[i] = moved
            if step < 3:
                hi, lo = split(image)
                left[0:16, span(i)] = hi
                left[16:32, span(i)] = lo
            if step == 2:
                hi, lo = split(moved)
                left[32:48, span(i)] = hi
                left[48:64, span(i)] = lo
        if step < 3:
            out = h3out.at[step - 1]
            for s in range(2):
                out[s] = ad[iface[s]]
            halo(step + 2, out, h3in.at[step - 1])

    def with_qxd(rows):
        gram = mm_nt(left[0 : 2 * rows], right[0:64])
        gram = gram[0:rows] + gram[rows : 2 * rows]
        return gram[:, 0:32] + gram[:, 32:64]

    residual(1)
    gram = with_qxd(16)
    spread(ar_small.at[0], 0, 2, pack4(gram))

    spread(ar_extra.at[1], 1, 4, gathered(ar_extra.at[0], 0, 4))
    total = unpack2(gathered(ar_big.at[1], 1, 1)) * scale
    kp, kq_mp, mq = total[:, 0:32], total[:, 32:64], total[:, 64:96]
    image = -RELAX * (
        small(inv_v, kp) - theta * (small(inv_v, kq_mp) - theta * small(inv_v, mq))
    )
    p_x = 2.0 * start_x - RELAX * image[:, 16:32] + RELAX * small(r, g_px)

    def advance(image, r_m, p_x):
        m = small(image[:, 0:16], gram_m) - r_m
        r = small(p_x, gram_v) + RELAX * small(m, qx_v)
        return m, p_x + RELAX * small(m, g_qx), r

    def coefficients(m, r):
        parts = [
            start_p + RELAX * r,
            start_q + RELAX * m,
            -RELAX * RELAX * m,
            RELAX * RELAX * theta * m,
        ]
        return jnp.concatenate(parts, axis=1)

    def image_of(m):
        return RELAX * (small(m, kq) - theta * small(m, mq))

    for step in (1, 2):
        m, c_x, r = advance(image, r_m, p_x)
        coef = coefficients(m, r)
        for t in range(TILES):
            p = pt[t] - RELAX * ad[t] + combine(coef, 64, t)
            pt[t] = p
            hi, lo = split(p)
            ext16[t, 0:16] = hi
            ext16[t, 16:32] = lo
        for t in range(TILES, EXT):
            pt[t] = pt[t] + combine(coef, 64, t)
        if step == 2:
            spread(ar_third.at[1], 1, 3, gathered(ar_third.at[0], 0, 3))
        halo_wait(step + 2, h3in.at[step - 1])
        for g in range(3):
            for s in range(2):
                t = TILES + 2 * g + s
                p = pt[t] - RELAX * h3in[step - 1, g, s]
                pt[t] = p
                hi, lo = split(p)
                ext16[t, 0:16] = hi
                ext16[t, 16:32] = lo
        residual(step + 1)
        r_px = small(r, g_px)
        r_m = small(r, pq_m)
        if step == 1:
            gram = with_qxd(16)
            gram_b = with_back(left[32:64], 16)
            gram_b = gram_b[:, 0:32] - theta * gram_b[:, 32:64]
            spread(ar_third.at[0], 0, 3, jnp.stack([pack4(gram), pack4(gram_b)]))
            extra = unpack2(gathered(ar_extra.at[1], 1, 4)) * scale
            kq = extra[:, 96:128]
            mp = kq_mp - kq
            m_image = image_of(m)
            image = unpack4(gathered(ar_small.at[1], 1, 2)) * scale + m_image
            p_x = c_x + start_x - RELAX * image[:, 16:32] + RELAX * r_px

    m_image = image_of(m)
    near = coef[:, 0:32]
    twice = small(m, extra[:, 0:32]) - theta * (
        small(m, extra[:, 32:64]) - theta * small(m, extra[:, 64:96])
    )
    known = small(near, jnp.concatenate([kp, kq], axis=0)) - theta * small(
        near, jnp.concatenate([mp, mq], axis=0)
    )
    known = known - RELAX * RELAX * twice
    total = gathered(ar_third.at[1], 1, 3) * scale
    image = unpack4(total[0])
    known = known + image - RELAX * unpack4(total[1])
    image = image + m_image
    p_x = c_x + start_x - RELAX * image[:, 16:32] + RELAX * r_px
    m, c_x, r = advance(image, r_m, p_x)
    coef = coefficients(m, r)
    image = known + image_of(m)
    r_m = small(r, pq_m)
    p_x = c_x + start_x - RELAX * image[:, 16:32] + RELAX * small(r, g_px)
    for t in range(TILES):
        pt[t] = pt[t] - RELAX * ad[t] + combine(coef, 64, t)

    m, c_x, r = advance(image, r_m, p_x)
    q_hi, q_lo = split(RELAX * m)
    x_hi, x_lo = split(-r)
    lead = jnp.concatenate([q_hi, x_hi], axis=1)
    rest = jnp.concatenate([q_lo, x_lo], axis=1)
    for t in range(TILES):
        hi = jnp.concatenate([s_hi[t, 16:32], right[64:80, span(t)]], axis=0)
        lo = jnp.concatenate([s_lo[t, 16:32], right[80:96, span(t)]], axis=0)
        out_ref[:, span(t)] = pt[t] + (mm(lead, hi) + mm(rest, hi) + mm(lead, lo))

    for step, out in enumerate((h0out, h1out, h2out, h3out.at[0], h3out.at[1])):
        for g in range(3):
            pltpu.make_async_copy(out, out, hs_sem.at[step]).wait()
    sent = adj.at[pl.ds(TILES, 6)]
    pltpu.make_async_copy(sent, sent, hs_sem.at[5]).wait()
    for step, buf in enumerate((ar_first, ar_big, ar_small, ar_third, ar_extra)):
        for stage in range(2):
            most = buf.at[stage, pl.ds(0, GROUP - 1)]
            pltpu.make_async_copy(most, most, as_sem.at[2 * step + stage]).wait()


def shards(basis, k_tiles, m_tiles, tile_part, tile_slot, iface_rows):
    rows = basis.shape[1] * lax.axis_size(AXIS)
    vmem = pltpu.VMEM
    corrections, theta = pl.pallas_call(
        functools.partial(kernel, 1.0 / rows),
        out_shape=(
            pltpu.VMEM((PAIRS, LOCAL), F32),
            pltpu.VMEM((1, PAIRS), F32),
        ),
        in_specs=[pl.BlockSpec(memory_space=pltpu.HBM)] * 6,
        out_specs=(pl.BlockSpec(memory_space=vmem), pl.BlockSpec(memory_space=vmem)),
        scratch_shapes=[
            vmem((TILES, BLOCKS, WIDTH, WIDTH), F32),
            vmem((TILES, BLOCKS, WIDTH, WIDTH), F32),
            vmem((TILES, BLOCKS * WIDTH, 2 * WIDTH), BF16),
            vmem((TILES, BLOCKS * WIDTH, 2 * WIDTH), BF16),
            vmem((TILES, 16, WIDTH), F32),
            vmem((TILES, 8, WIDTH), F32),
            vmem((EXT, 32, WIDTH), BF16),
            vmem((EXT, 64, WIDTH), BF16),
            vmem((TILES, 96, WIDTH), F32),
            vmem((EXT, 96, WIDTH), BF16),
            vmem((EXT, 96, WIDTH), BF16),
            vmem((EXT, 16, WIDTH), F32),
            vmem((TILES, 16, WIDTH), F32),
            vmem((96, LOCAL), BF16),
            vmem((128, LOCAL), BF16),
            vmem((2, 16, WIDTH), F32),
            vmem((2, 32, WIDTH), F32),
            vmem((2, 64, WIDTH), F32),
            vmem((2, 2, 16, WIDTH), F32),
            vmem((3, 2, 16, WIDTH), F32),
            vmem((3, 2, 32, WIDTH), F32),
            vmem((3, 2, 64, WIDTH), F32),
            vmem((2, 3, 2, 16, WIDTH), F32),
            vmem((2, GROUP, 5, 2, WIDTH), F32),
            vmem((2, GROUP, 6, 2, WIDTH), F32),
            vmem((2, GROUP, 4, WIDTH), F32),
            vmem((2, GROUP, 2, 4, WIDTH), F32),
            vmem((2, GROUP, 8, 2, WIDTH), F32),
            vmem((TILES, BLOCKS, 64, WIDTH), F32),
            vmem((EXT, 64, WIDTH), F32),
            vmem((3, 2, 64, WIDTH), F32),
            vmem((128, LOCAL), BF16),
            pltpu.SMEM((TILES, BLOCKS), jnp.int32),
            pltpu.SMEM((TILES, BLOCKS), jnp.int32),
            pltpu.SMEM((2,), jnp.int32),
            pltpu.SemaphoreType.DMA((2, TILES)),
            pltpu.SemaphoreType.DMA((3,)),
            pltpu.SemaphoreType.DMA((TILES,)),
            pltpu.SemaphoreType.DMA((6,)),
            pltpu.SemaphoreType.DMA((6,)),
            pltpu.SemaphoreType.DMA((10,)),
            pltpu.SemaphoreType.DMA((10,)),
        ],
        compiler_params=pltpu.CompilerParams(
            collective_id=0, has_side_effects=True, vmem_limit_bytes=60 * 1024 * 1024
        ),
    )(basis, k_tiles, m_tiles, tile_part, tile_slot, iface_rows)
    return corrections, theta.reshape(PAIRS)


def solution(mesh):
    in_specs = (
        P(None, AXIS),
        P(AXIS, None, None, None),
        P(AXIS, None, None, None),
        P(AXIS, None),
        P(AXIS, None),
        P(AXIS),
    )
    return jax.shard_map(
        shards, mesh=mesh, in_specs=in_specs, out_specs=(P(None, AXIS), P()), check_vma=False
    )
```

```python
import functools

import jax
import jax.numpy as jnp
from jax import lax
from jax.experimental import pallas as pl
from jax.experimental.pallas import tpu as pltpu
from jax.sharding import PartitionSpec as P

AXIS = "parts"
PARTS = 256
GROUP = 16
FAR = 128
PAIRS = 16
TILES = 8
BLOCKS = 5
WIDTH = 128
LOCAL = TILES * WIDTH
EXT = TILES + 6
RELAX = 0.4
MESH = pl.DeviceIdType.MESH
ORDER_A = (8, 7, 9, 6, 10, 5, 11, 4, 12, 3, 13, 2, 14, 1, 15)
ORDER_B = (10, 6, 14, 9, 11, 2, 8, 5, 7, 13, 15, 1, 3, 4, 12)
F32 = jnp.float32
BF16 = jnp.bfloat16
NT = (((1,), (1,)), ((), ()))
TN = (((0,), (0,)), ((), ()))


def split(x):
    hi = x.astype(BF16)
    return hi, (x - hi.astype(F32)).astype(BF16)


def mm(a, b):
    return jnp.dot(a, b, preferred_element_type=F32)


def mm_nt(a, b):
    return lax.dot_general(a, b, NT, preferred_element_type=F32)


def small(a, b, dims=(((1,), (0,)), ((), ()))):
    return lax.dot_general(
        a, b, dims, precision=lax.Precision.HIGHEST, preferred_element_type=F32
    )


def pack4(v):
    return jnp.concatenate([v[4 * i : 4 * i + 4] for i in range(4)], axis=1)


def unpack4(v):
    return jnp.concatenate([v[:, 32 * i : 32 * i + 32] for i in range(4)], axis=0)


def pack2(v):
    flat = jnp.concatenate([v[2 * i : 2 * i + 2] for i in range(8)], axis=1)
    return jnp.stack([flat[:, WIDTH * u : WIDTH * u + WIDTH] for u in range(v.shape[1] // 16)])


def unpack2(v):
    flat = jnp.concatenate([v[u] for u in range(v.shape[0])], axis=1)
    wide = 16 * v.shape[0]
    return jnp.concatenate([flat[:, wide * i : wide * i + wide] for i in range(8)], axis=0)


def eliminate(gram, rows, eye):
    aug = jnp.concatenate([gram, eye], axis=1)
    for j in range(PAIRS):
        pivot = aug[j : j + 1, j : j + 1]
        d = lax.rsqrt(pivot)
        d = d * (1.5 - 0.5 * pivot * d * d)
        line = aug[j : j + 1, :] * d
        col = aug[:, j : j + 1] * d
        aug = jnp.where(rows == j, line, jnp.where(rows > j, aug - col * line, aug))
    return aug[:, PAIRS:]


def kernel(
    scale,
    basis_ref,
    k_ref,
    m_ref,
    part_hbm,
    slot_hbm,
    iface_hbm,
    out_ref,
    theta_ref,
    kbuf,
    mbuf,
    w_hi,
    w_lo,
    xt,
    dinv,
    ext16,
    ext32,
    words,
    s_hi,
    s_lo,
    pt,
    ad,
    right,
    left,
    h0out,
    h1out,
    h2out,
    h3out,
    h0in,
    h1in,
    h2in,
    h3in,
    ar_first,
    ar_big,
    ar_small,
    ar_third,
    ar_extra,
    back,
    adj,
    zin,
    right2,
    part_ref,
    slot_ref,
    iface_ref,
    load_sem,
    index_sem,
    x_sem,
    hs_sem,
    hr_sem,
    as_sem,
    ar_sem,
):
    me = lax.axis_index(AXIS)
    rank_a = lax.rem(me, GROUP)
    base_a = me - rank_a
    rank_b = me // GROUP
    halo_to = (
        lax.rem(me + PARTS - 1, PARTS),
        lax.rem(me + 1, PARTS),
        lax.rem(me + FAR, PARTS),
    )

    def peer_a(k):
        return base_a + lax.rem(rank_a + k, GROUP)

    def peer_b(k):
        across = lax.rem(lax.rem(rank_b, 4) + k % 4, 4)
        along = lax.rem(rank_b // 4 + k // 4, 4)
        return rank_a + GROUP * (4 * along + across)

    loads = []
    tables = ((part_hbm, part_ref), (slot_hbm, slot_ref), (iface_hbm, iface_ref))
    for n, (src, dst) in enumerate(tables):
        loads.append(pltpu.make_async_copy(src, dst, index_sem.at[n]))
        loads[-1].start()
    for i in range(TILES):
        loads.append(
            pltpu.make_async_copy(
                basis_ref.at[:, pl.ds(i * WIDTH, WIDTH)], xt.at[i], x_sem.at[i]
            )
        )
        loads[-1].start()
    barrier = pltpu.get_barrier_semaphore()

    for near, far in zip(ORDER_A, ORDER_B):
        for device in (peer_b(far), peer_a(near)):
            pl.semaphore_signal(barrier, inc=1, device_id=(device,), device_id_type=MESH)
    for device in halo_to:
        pl.semaphore_signal(barrier, inc=1, device_id=(device,), device_id_type=MESH)

    for i in range(TILES):
        for n, (src, dst) in enumerate(((k_ref, kbuf), (m_ref, mbuf))):
            pltpu.make_async_copy(src.at[i], dst.at[i], load_sem.at[n, i]).start()

    def halo(step, out, into):
        for g, device in enumerate(halo_to):
            pltpu.make_async_remote_copy(
                src_ref=out,
                dst_ref=into.at[g],
                send_sem=hs_sem.at[step],
                recv_sem=hr_sem.at[step],
                device_id=(device,),
                device_id_type=MESH,
            ).start()

    def halo_wait(step, into):
        pltpu.make_async_copy(into, into, hr_sem.at[step]).wait()

    def spread(buf, stage, step, value):
        rank = rank_a if stage == 0 else rank_b
        peer = peer_a if stage == 0 else peer_b
        buf[rank] = value

        for k in ORDER_A if stage == 0 else ORDER_B:
            pltpu.make_async_remote_copy(
                src_ref=buf.at[rank],
                dst_ref=buf.at[rank],
                send_sem=as_sem.at[2 * step + stage],
                recv_sem=ar_sem.at[2 * step + stage],
                device_id=(peer(k),),
                device_id_type=MESH,
            ).start()

    def gathered(buf, stage, step):
        most = buf.at[pl.ds(0, GROUP - 1)]
        pltpu.make_async_copy(most, most, ar_sem.at[2 * step + stage]).wait()
        total = buf[0]
        for j in range(1, GROUP):
            total = total + buf[j]
        return total

    def span(i):
        return pl.ds(i * WIDTH, WIDTH)

    for copy in loads:
        copy.wait()
    columns = []
    for i in range(TILES):
        line = []
        for b in range(BLOCKS):
            part = part_ref[i, b]
            slot = slot_ref[i, b]
            where = jnp.where(
                part == halo_to[1],
                TILES,
                jnp.where(part == halo_to[0], TILES + 2, TILES + 4),
            )
            line.append(jnp.where(part == me, slot, where + slot))
        columns.append(line)
    iface = [iface_ref[0], iface_ref[1]]
    for s in range(2):
        h0out[s] = xt[iface[s]]
    pl.semaphore_wait(barrier, 33)
    halo(0, h0out, h0in)

    eye_w = lax.broadcasted_iota(jnp.int32, (WIDTH, WIDTH), 0) == lax.broadcasted_iota(
        jnp.int32, (WIDTH, WIDTH), 1
    )
    for i in range(TILES):
        hi, lo = split(xt[i])
        ext16[i, 0:16] = hi
        ext16[i, 16:32] = lo
        right[64:80, span(i)] = hi
        right[80:96, span(i)] = lo
        left[0:16, span(i)] = hi
        left[48:64, span(i)] = lo

    def prepare(i, carry):
        for n, (src, dst) in enumerate(((k_ref, kbuf), (m_ref, mbuf))):
            pltpu.make_async_copy(src.at[i], dst.at[i], load_sem.at[n, i]).wait()
            for b in range(BLOCKS):
                hi, lo = split(dst[i, b].T)
                w_hi[i, b * WIDTH : (b + 1) * WIDTH, n * WIDTH : (n + 1) * WIDTH] = hi
                w_lo[i, b * WIDTH : (b + 1) * WIDTH, n * WIDTH : (n + 1) * WIDTH] = lo
        diagonal = jnp.sum(jnp.where(eye_w, kbuf[i, 0], 0.0), axis=0, keepdims=True)
        dinv[i] = jnp.broadcast_to(1.0 / diagonal, (8, WIDTH))
        return carry

    lax.fori_loop(0, TILES, prepare, 0)
    d = [dinv[i, 0:1] for i in range(TILES)]
    for i in range(TILES):
        hi, lo = split(xt[i] * d[i])
        right[16:32, span(i)] = hi
        right[48:64, span(i)] = lo

    def apply(ext, rows, i):
        picked = jnp.concatenate([ext[columns[i][b]] for b in range(BLOCKS)], axis=1)
        high = mm(picked, w_hi[i])
        low = mm(picked[:rows], w_lo[i])
        return high[:rows] + high[rows:] + low

    halo_wait(0, h0in)
    for g in range(3):
        for s in range(2):
            hi, lo = split(h0in[g, s])
            ext16[TILES + 2 * g + s, 0:16] = hi
            ext16[TILES + 2 * g + s, 16:32] = lo
    for i in range(TILES):
        y = apply(ext16, 16, i)
        p, q = y[:, :WIDTH], y[:, WIDTH:]
        words[i, 0:16] = p * d[i]
        words[i, 16:32] = q * d[i]
        hi, lo = split(p)
        left[16:32, span(i)] = hi
        left[64:80, span(i)] = lo
        hi, lo = split(q)
        left[32:48, span(i)] = hi
        left[80:96, span(i)] = lo
        right[0:16, span(i)] = hi
        right[32:48, span(i)] = lo
    for s in range(2):
        h1out[s] = words[iface[s], 0:32]
    halo(1, h1out, h1in)

    gram = mm_nt(left[0:96], right[...])
    gram = gram[0:48] + gram[48:96]
    with_qx = gram[:, 0:32] + gram[:, 32:64]
    with_x = gram[:, 64:80] + gram[:, 80:96]
    payload = pack2(
        jnp.concatenate([with_qx[16:32], with_qx[32:48], with_x[0:16]], axis=1)
    )
    spread(ar_first.at[0], 0, 0, payload)

    for i in range(TILES):
        hi, lo = split(words[i, 0:32])
        ext32[i, 0:32] = hi
        ext32[i, 32:64] = lo
        s_hi[i, 0:32] = hi
        s_lo[i, 0:32] = lo
    for i in range(TILES):
        hi, lo = right[0:32, span(i)], right[32:64, span(i)]
        none = jnp.zeros((32, WIDTH), BF16)
        hi = jnp.concatenate(
            [jnp.concatenate([hi, none], axis=1), jnp.concatenate([none, hi], axis=1)], axis=0
        )
        lo = jnp.concatenate(
            [jnp.concatenate([lo, none], axis=1), jnp.concatenate([none, lo], axis=1)], axis=0
        )
        high = mm_nt(jnp.concatenate([hi, lo], axis=0), w_hi[i])
        share = high[0:64] + high[64:128] + mm_nt(hi, w_lo[i])
        for b in range(BLOCKS):
            back[i, b] = share[:, b * WIDTH : (b + 1) * WIDTH]

    def collect(j, total):
        for i in range(TILES):
            for b in range(1, BLOCKS):
                total = total + jnp.where(columns[i][b] == j, back[i, b], 0.0)
        adj[j] = total

    def collect_remote(j, carry):
        collect(j, jnp.zeros((64, WIDTH), F32))
        return carry

    def collect_local(j, carry):
        collect(j, back[j, 0])
        return carry

    lax.fori_loop(TILES, EXT, collect_remote, 0)
    for g, device in enumerate((halo_to[1], halo_to[0], halo_to[2])):
        pltpu.make_async_remote_copy(
            src_ref=adj.at[pl.ds(TILES + 2 * g, 2)],
            dst_ref=zin.at[g],
            send_sem=hs_sem.at[5],
            recv_sem=hr_sem.at[5],
            device_id=(device,),
            device_id_type=MESH,
        ).start()
    halo_wait(1, h1in)
    for g in range(3):
        for s in range(2):
            hi, lo = split(h1in[g, s])
            t = TILES + 2 * g + s
            ext32[t, 0:32] = hi
            ext32[t, 32:64] = lo
            s_hi[t, 0:32] = hi
            s_lo[t, 0:32] = lo

    for i in range(TILES):
        if i == 0:
            spread(ar_first.at[1], 1, 0, gathered(ar_first.at[0], 0, 0))
        y = apply(ext32, 32, i)
        stiff, mass = y[:, :WIDTH], y[:, WIDTH:]
        hi, lo = split(stiff)
        left[0:32, span(i)] = hi
        left[64:96, span(i)] = lo
        hi, lo = split(mass)
        left[32:64, span(i)] = hi
        left[96:128, span(i)] = lo
        stiff, mass = stiff * d[i], mass * d[i]
        words[i, 32:48] = stiff[16:32]
        words[i, 48:64] = mass[16:32]
        words[i, 64:80] = stiff[0:16]
        words[i, 80:96] = mass[0:16]
    for s in range(2):
        h2out[s] = words[iface[s], 32:96]
    halo(2, h2out, h2in)
    gram = mm_nt(left[...], right[0:64])
    gram = gram[0:64] + gram[64:128]
    gram = gram[:, 0:32] + gram[:, 32:64]
    kept = gram[16:32]
    payload = pack2(jnp.concatenate([gram[0:16], kept + gram[32:48], gram[48:64]], axis=1))
    spread(ar_big.at[0], 0, 1, payload)
    for i in range(TILES):
        hi, lo = split(words[i, 32:96])
        s_hi[i, 32:96] = hi
        s_lo[i, 32:96] = lo
    lax.fori_loop(0, TILES, collect_local, 0)

    def with_back(both, rows):
        gram = mm_nt(both, right2[...])
        gram = gram[0:rows] + gram[rows : 2 * rows]
        return gram[:, 0:64] + gram[:, 64:128]

    pltpu.make_async_copy(zin, zin, hr_sem.at[5]).wait()
    for j in range(TILES):
        total = adj[j]
        for s in range(2):
            for g in range(3):
                total = total + jnp.where(iface[s] == j, zin[g, s], 0.0)
        hi, lo = split(total)
        right2[0:64, span(j)] = hi
        right2[64:128, span(j)] = lo
    both = jnp.concatenate(
        [
            jnp.concatenate([s_hi[t, 32:64] for t in range(TILES)], axis=1),
            jnp.concatenate([s_lo[t, 32:64] for t in range(TILES)], axis=1),
        ],
        axis=0,
    )
    gram = with_back(both, 32)
    middle = gram[0:16, 32:64] + gram[16:32, 0:32]
    spread(
        ar_extra.at[0],
        0,
        4,
        pack2(jnp.concatenate([gram[0:16, 0:32], middle, gram[16:32, 32:64], kept], axis=1)),
    )


    total = gathered(ar_first.at[1], 1, 0) * scale
    total = unpack2(total)
    g_p, g_q, g_xx = total[:, 0:32], total[:, 32:64], total[:, 64:80]
    g_pq, g_px = g_p[:, 0:16], g_p[:, 16:32]
    g_qq, g_qx = g_q[:, 0:16], g_q[:, 16:32]
    row_no = lax.broadcasted_iota(jnp.int32, (PAIRS, 2 * PAIRS), 0)
    eye_b = lax.broadcasted_iota(jnp.int32, (PAIRS, PAIRS), 0) == lax.broadcasted_iota(
        jnp.int32, (PAIRS, PAIRS), 1
    )
    eye = jnp.where(eye_b, 1.0, 0.0).astype(F32)
    inv_v = eliminate(g_xx, row_no, eye)
    inv_m = eliminate(g_qq, row_no, eye)
    projected = small(inv_m, g_pq, NT)
    diag_v = jnp.sum(jnp.where(eye_b, inv_v, 0.0), axis=1, keepdims=True)
    diag_m = jnp.sum(jnp.where(eye_b, inv_m, 0.0), axis=1, keepdims=True)
    theta = jnp.sum(projected * inv_v, axis=1, keepdims=True) * diag_m / diag_v
    theta_ref[...] = jnp.sum(jnp.where(eye_b, theta, 0.0), axis=0, keepdims=True)
    wide = jnp.broadcast_to(theta, (PAIRS, WIDTH))
    gram_v = small(inv_v, inv_v, TN)
    gram_m = small(inv_m, inv_m, TN)
    start_p = -RELAX * inv_v
    start_q = RELAX * theta * inv_v
    start_x = small(start_p, g_px) + small(start_q, g_qx)
    r = small(start_x, gram_v)
    pq_m = small(g_pq, gram_m)
    qx_v = small(g_qx, gram_v)
    r_m = small(r, pq_m)
    coef = jnp.concatenate(
        [
            2.0 * start_p + RELAX * r,
            2.0 * start_q,
            -RELAX * start_q,
            RELAX * theta * start_q,
            -RELAX * start_p,
            RELAX * theta * start_p,
        ],
        axis=1,
    )
    halo_wait(2, h2in)
    for g in range(3):
        for s in range(2):
            hi, lo = split(h2in[g, s])
            t = TILES + 2 * g + s
            s_hi[t, 32:96] = hi
            s_lo[t, 32:96] = lo

    def combine(coef, rows, t):
        hi, lo = split(coef)
        both = jnp.concatenate([hi, lo], axis=0)
        first = mm(both, s_hi[t, 0:rows])
        second = mm(hi, s_lo[t, 0:rows])
        return first[0:16] + first[16:32] + second

    for t in range(EXT):
        p = combine(coef, 96, t)
        pt[t] = p
        hi, lo = split(p)
        ext16[t, 0:16] = hi
        ext16[t, 16:32] = lo

    def residual(step):
        for i in range(TILES):
            if i == 4 and step == 1:
                spread(ar_big.at[1], 1, 1, gathered(ar_big.at[0], 0, 1))
            if i == 4 and step == 2:
                spread(ar_small.at[1], 1, 2, gathered(ar_small.at[0], 0, 2))
            y = apply(ext16, 16, i)
            image = y[:, :WIDTH] - wide * y[:, WIDTH:]
            moved = image * d[i]
            ad[i] = moved
            if step < 3:
                hi, lo = split(image)
                left[0:16, span(i)] = hi
                left[16:32, span(i)] = lo
            if step == 2:
                hi, lo = split(moved)
                left[32:48, span(i)] = hi
                left[48:64, span(i)] = lo
        if step < 3:
            out = h3out.at[step - 1]
            for s in range(2):
                out[s] = ad[iface[s]]
            halo(step + 2, out, h3in.at[step - 1])

    def with_qxd(rows):
        gram = mm_nt(left[0 : 2 * rows], right[0:64])
        gram = gram[0:rows] + gram[rows : 2 * rows]
        return gram[:, 0:32] + gram[:, 32:64]

    residual(1)
    gram = with_qxd(16)
    spread(ar_small.at[0], 0, 2, pack4(gram))

    spread(ar_extra.at[1], 1, 4, gathered(ar_extra.at[0], 0, 4))
    total = unpack2(gathered(ar_big.at[1], 1, 1)) * scale
    kp, kq_mp, mq = total[:, 0:32], total[:, 32:64], total[:, 64:96]
    image = -RELAX * (
        small(inv_v, kp) - theta * (small(inv_v, kq_mp) - theta * small(inv_v, mq))
    )
    p_x = 2.0 * start_x - RELAX * image[:, 16:32] + RELAX * small(r, g_px)

    def advance(image, r_m, p_x):
        m = small(image[:, 0:16], gram_m) - r_m
        r = small(p_x, gram_v) + RELAX * small(m, qx_v)
        return m, p_x + RELAX * small(m, g_qx), r

    def coefficients(m, r):
        parts = [
            start_p + RELAX * r,
            start_q + RELAX * m,
            -RELAX * RELAX * m,
            RELAX * RELAX * theta * m,
        ]
        return jnp.concatenate(parts, axis=1)

    def image_of(m):
        return RELAX * (small(m, kq) - theta * small(m, mq))

    for step in (1, 2):
        m, c_x, r = advance(image, r_m, p_x)
        coef = coefficients(m, r)
        for t in range(TILES):
            p = pt[t] - RELAX * ad[t] + combine(coef, 64, t)
            pt[t] = p
            hi, lo = split(p)
            ext16[t, 0:16] = hi
            ext16[t, 16:32] = lo
        for t in range(TILES, EXT):
            pt[t] = pt[t] + combine(coef, 64, t)
        if step == 2:
            spread(ar_third.at[1], 1, 3, gathered(ar_third.at[0], 0, 3))
        halo_wait(step + 2, h3in.at[step - 1])
        for g in range(3):
            for s in range(2):
                t = TILES + 2 * g + s
                p = pt[t] - RELAX * h3in[step - 1, g, s]
                pt[t] = p
                hi, lo = split(p)
                ext16[t, 0:16] = hi
                ext16[t, 16:32] = lo
        residual(step + 1)
        r_px = small(r, g_px)
        r_m = small(r, pq_m)
        if step == 1:
            gram = with_qxd(16)
            gram_b = with_back(left[32:64], 16)
            gram_b = gram_b[:, 0:32] - theta * gram_b[:, 32:64]
            spread(ar_third.at[0], 0, 3, jnp.stack([pack4(gram), pack4(gram_b)]))
            extra = unpack2(gathered(ar_extra.at[1], 1, 4)) * scale
            kq = extra[:, 96:128]
            mp = kq_mp - kq
            m_image = image_of(m)
            image = unpack4(gathered(ar_small.at[1], 1, 2)) * scale + m_image
            p_x = c_x + start_x - RELAX * image[:, 16:32] + RELAX * r_px

    m_image = image_of(m)
    near = coef[:, 0:32]
    twice = small(m, extra[:, 0:32]) - theta * (
        small(m, extra[:, 32:64]) - theta * small(m, extra[:, 64:96])
    )
    known = small(near, jnp.concatenate([kp, kq], axis=0)) - theta * small(
        near, jnp.concatenate([mp, mq], axis=0)
    )
    known = known - RELAX * RELAX * twice
    total = gathered(ar_third.at[1], 1, 3) * scale
    image = unpack4(total[0])
    known = known + image - RELAX * unpack4(total[1])
    image = image + m_image
    p_x = c_x + start_x - RELAX * image[:, 16:32] + RELAX * r_px
    m, c_x, r = advance(image, r_m, p_x)
    coef = coefficients(m, r)
    image = known + image_of(m)
    r_m = small(r, pq_m)
    p_x = c_x + start_x - RELAX * image[:, 16:32] + RELAX * small(r, g_px)
    for t in range(TILES):
        pt[t] = pt[t] - RELAX * ad[t] + combine(coef, 64, t)

    m, c_x, r = advance(image, r_m, p_x)
    q_hi, q_lo = split(RELAX * m)
    x_hi, x_lo = split(-r)
    lead = jnp.concatenate([q_hi, x_hi], axis=1)
    rest = jnp.concatenate([q_lo, x_lo], axis=1)
    for t in range(TILES):
        hi = jnp.concatenate([s_hi[t, 16:32], right[64:80, span(t)]], axis=0)
        lo = jnp.concatenate([s_lo[t, 16:32], right[80:96, span(t)]], axis=0)
        out_ref[:, span(t)] = pt[t] + (mm(lead, hi) + mm(rest, hi) + mm(lead, lo))

    for step, out in enumerate((h0out, h1out, h2out, h3out.at[0], h3out.at[1])):
        for g in range(3):
            pltpu.make_async_copy(out, out, hs_sem.at[step]).wait()
    sent = adj.at[pl.ds(TILES, 6)]
    pltpu.make_async_copy(sent, sent, hs_sem.at[5]).wait()
    for step, buf in enumerate((ar_first, ar_big, ar_small, ar_third, ar_extra)):
        for stage in range(2):
            most = buf.at[stage, pl.ds(0, GROUP - 1)]
            pltpu.make_async_copy(most, most, as_sem.at[2 * step + stage]).wait()


def shards(basis, k_tiles, m_tiles, tile_part, tile_slot, iface_rows):
    rows = basis.shape[1] * lax.axis_size(AXIS)
    vmem = pltpu.VMEM
    corrections, theta = pl.pallas_call(
        functools.partial(kernel, 1.0 / rows),
        out_shape=(
            pltpu.VMEM((PAIRS, LOCAL), F32),
            pltpu.VMEM((1, PAIRS), F32),
        ),
        in_specs=[pl.BlockSpec(memory_space=pltpu.HBM)] * 6,
        out_specs=(pl.BlockSpec(memory_space=vmem), pl.BlockSpec(memory_space=vmem)),
        scratch_shapes=[
            vmem((TILES, BLOCKS, WIDTH, WIDTH), F32),
            vmem((TILES, BLOCKS, WIDTH, WIDTH), F32),
            vmem((TILES, BLOCKS * WIDTH, 2 * WIDTH), BF16),
            vmem((TILES, BLOCKS * WIDTH, 2 * WIDTH), BF16),
            vmem((TILES, 16, WIDTH), F32),
            vmem((TILES, 8, WIDTH), F32),
            vmem((EXT, 32, WIDTH), BF16),
            vmem((EXT, 64, WIDTH), BF16),
            vmem((TILES, 96, WIDTH), F32),
            vmem((EXT, 96, WIDTH), BF16),
            vmem((EXT, 96, WIDTH), BF16),
            vmem((EXT, 16, WIDTH), F32),
            vmem((TILES, 16, WIDTH), F32),
            vmem((96, LOCAL), BF16),
            vmem((128, LOCAL), BF16),
            vmem((2, 16, WIDTH), F32),
            vmem((2, 32, WIDTH), F32),
            vmem((2, 64, WIDTH), F32),
            vmem((2, 2, 16, WIDTH), F32),
            vmem((3, 2, 16, WIDTH), F32),
            vmem((3, 2, 32, WIDTH), F32),
            vmem((3, 2, 64, WIDTH), F32),
            vmem((2, 3, 2, 16, WIDTH), F32),
            vmem((2, GROUP, 5, 2, WIDTH), F32),
            vmem((2, GROUP, 6, 2, WIDTH), F32),
            vmem((2, GROUP, 4, WIDTH), F32),
            vmem((2, GROUP, 2, 4, WIDTH), F32),
            vmem((2, GROUP, 8, 2, WIDTH), F32),
            vmem((TILES, BLOCKS, 64, WIDTH), F32),
            vmem((EXT, 64, WIDTH), F32),
            vmem((3, 2, 64, WIDTH), F32),
            vmem((128, LOCAL), BF16),
            pltpu.SMEM((TILES, BLOCKS), jnp.int32),
            pltpu.SMEM((TILES, BLOCKS), jnp.int32),
            pltpu.SMEM((2,), jnp.int32),
            pltpu.SemaphoreType.DMA((2, TILES)),
            pltpu.SemaphoreType.DMA((3,)),
            pltpu.SemaphoreType.DMA((TILES,)),
            pltpu.SemaphoreType.DMA((6,)),
            pltpu.SemaphoreType.DMA((6,)),
            pltpu.SemaphoreType.DMA((10,)),
            pltpu.SemaphoreType.DMA((10,)),
        ],
        compiler_params=pltpu.CompilerParams(
            collective_id=0, has_side_effects=True, vmem_limit_bytes=60 * 1024 * 1024
        ),
    )(basis, k_tiles, m_tiles, tile_part, tile_slot, iface_rows)
    return corrections, theta.reshape(PAIRS)


def solution(mesh):
    in_specs = (
        P(None, AXIS),
        P(AXIS, None, None, None),
        P(AXIS, None, None, None),
        P(AXIS, None),
        P(AXIS, None),
        P(AXIS),
    )
    return jax.shard_map(
        shards, mesh=mesh, in_specs=in_specs, out_specs=(P(None, AXIS), P()), check_vma=False
    )
```
